16 devices in a mesh: dp: 2 (over y, z), ep: 8 (over x, core).
Axes of the slice: x: 4, y: 2, z: 1, core: 2. Of those that a mesh axis runs over, the one named last changes fastest.
The devices are a block of a 4x4x8 slice.
Arguments:
- tokens: bfloat16 [131072, 768], P(('dp', 'ep')), parts along dimension 0
- choice_idx: int32 [64, 2048], P(('dp', 'ep')), parts along dimension 0
- gate_weight: float32 [64, 2048], P(('dp', 'ep')), parts along dimension 0
- w_in: bfloat16 [32, 768, 3072], P('ep')
- w_out: bfloat16 [32, 3072, 768], P('ep')
Outputs:
- output: bfloat16 [131072, 768], P(('dp', 'ep')), parts along dimension 0
There are 2 independent parts. The reference program is written for one: setup_inputs(seed, part) draws one part's arguments, and reference() takes and returns one part's arrays. A program takes and returns all parts, laid end to end along the dimension named above; an argument that names none is the same for every part.
All inputs are finite; a program needn't handle non-finite values.
Results may differ from the reference program's by a relative error of at most 0.001.
Values are sent between devices in bfloat16 or wider.
A program may use at most 768 MiB of HBM per device.

```python
import jax
import jax.numpy as jnp
from jax import lax

D_MODEL = 768
D_FF = 3072
EXPERTS = 32
TOKENS = 65536
CAPACITY = 2048
GROUP_SIZE = 8


def draw_routing(route_key):
    tok_local = TOKENS // GROUP_SIZE
    slots_dev = (EXPERTS // GROUP_SIZE) * CAPACITY
    base_share = slots_dev // GROUP_SIZE
    hot_rows = tok_local // 8
    cold_rows = tok_local - hot_rows
    half_group = GROUP_SIZE // 2
    route_keys = jax.random.split(route_key, 6)
    dev_grid = jnp.tile(jnp.arange(GROUP_SIZE, dtype=jnp.int32)[None, :], (GROUP_SIZE, 1))
    src_perm = jax.random.permutation(route_keys[0], dev_grid, axis=1, independent=True)
    pair_delta = jax.random.randint(route_keys[1], (GROUP_SIZE, half_group), 0, base_share + 1)
    pair_delta = pair_delta.at[:, 0].set(base_share)
    perm_counts = jnp.stack([base_share + pair_delta, base_share - pair_delta], axis=2).reshape(GROUP_SIZE, GROUP_SIZE)
    dest_ids = jnp.arange(GROUP_SIZE)[:, None]
    counts = jnp.zeros((GROUP_SIZE, GROUP_SIZE), jnp.int32).at[dest_ids, src_perm].set(perm_counts)
    block_ends = jnp.cumsum(counts, axis=1)
    starts = block_ends - counts
    slot_pos = jnp.arange(slots_dev, dtype=jnp.int32)
    src_of = jax.vmap(lambda end_row: jnp.searchsorted(end_row, slot_pos, side="right"))(block_ends)
    within = slot_pos[None, :] - jnp.take_along_axis(starts, src_of, axis=1)
    block_len = jnp.take_along_axis(counts, src_of, axis=1)
    hot_count = jnp.minimum(block_len // 2, hot_rows)
    hot_off = jax.random.randint(route_keys[2], (GROUP_SIZE, GROUP_SIZE), 0, hot_rows)
    cold_off = jax.random.randint(route_keys[3], (GROUP_SIZE, GROUP_SIZE), 0, cold_rows)
    hot_pick = (jnp.take_along_axis(hot_off, src_of, axis=1) + within) % hot_rows
    cold_pick = hot_rows + (jnp.take_along_axis(cold_off, src_of, axis=1) + within - hot_count) % cold_rows
    local_rank = jnp.where(within < hot_count, hot_pick, cold_pick)
    row_grid = jnp.tile(jnp.arange(tok_local, dtype=jnp.int32)[None, :], (GROUP_SIZE, 1))
    row_order = jax.random.permutation(route_keys[4], row_grid, axis=1, independent=True).reshape(-1)
    chosen = src_of * tok_local + row_order[src_of * tok_local + local_rank]
    chosen = chosen.reshape(EXPERTS, CAPACITY)
    return jax.random.permutation(route_keys[5], chosen, axis=1, independent=True)


def setup_inputs(seed: int = 0, part: int = 0) -> dict:
    base_key = jax.random.key(seed)
    shared_keys = jax.random.split(base_key, 2)
    part_keys = jax.random.split(jax.random.fold_in(base_key, part), 3)
    tokens = jax.random.normal(part_keys[0], (TOKENS, D_MODEL), jnp.float32).astype(jnp.bfloat16)
    choice_idx = draw_routing(part_keys[1])
    gate_weight = jax.random.uniform(part_keys[2], (EXPERTS, CAPACITY), jnp.float32, 0.5, 1.5)
    w_in = (jax.random.normal(shared_keys[0], (EXPERTS, D_MODEL, D_FF), jnp.float32) * D_MODEL ** -0.5).astype(jnp.bfloat16)
    w_out = (jax.random.normal(shared_keys[1], (EXPERTS, D_FF, D_MODEL), jnp.float32) * D_FF ** -0.5).astype(jnp.bfloat16)
    return {"tokens": tokens, "choice_idx": choice_idx, "gate_weight": gate_weight, "w_in": w_in, "w_out": w_out}


def reference(tokens, choice_idx, gate_weight, w_in, w_out):
    def expert_step(acc_sum, per_expert):
        idx_row, gate_row, w_first, w_second = per_expert
        tok_rows = tokens[idx_row]
        pre_act = jnp.dot(tok_rows, w_first, preferred_element_type=jnp.float32)
        hidden = jax.nn.gelu(pre_act, approximate=True).astype(jnp.bfloat16)
        expert_out = jnp.dot(hidden, w_second, preferred_element_type=jnp.float32)
        weighted = (gate_row[:, None] * expert_out).astype(jnp.bfloat16)
        return acc_sum.at[idx_row].add(weighted.astype(jnp.float32)), None

    zero_acc = jnp.zeros((TOKENS, D_MODEL), jnp.float32)
    acc_sum = lax.scan(expert_step, zero_acc, (choice_idx, gate_weight, w_in, w_out))[0]
    return (tokens.astype(jnp.float32) + acc_sum).astype(jnp.bfloat16)
```

```python
import functools

import jax
import jax.numpy as jnp
from jax import lax
from jax.experimental import pallas as pl
from jax.experimental.pallas import tpu as pltpu
from jax.sharding import PartitionSpec as P

LANES = 128
SUB = 8
GROUP = 16
VMEM_LIMIT = 62 * 1024 * 1024
CHUNKS = 4
ROW_TILE = 256


def load_table(tok_ref, raw, table, sems, rows):
    total, width = tok_ref.shape
    parts = total // rows
    copies = [
        pltpu.make_async_copy(tok_ref.at[pl.ds(p * rows, rows)], raw.at[pl.ds(p * rows, rows)], sems.at[p])
        for p in range(parts)
    ]
    for copy in copies:
        copy.start()
    for p in range(parts):
        copies[p].wait()

        def convert(g, carry):
            base = pl.multiple_of(p * rows + g * GROUP, GROUP)
            for k in range(width // LANES):
                x = raw[pl.ds(base, GROUP), k * LANES:(k + 1) * LANES].astype(jnp.float32)
                table[pl.ds(base * SUB + k, GROUP, stride=SUB), :] = x
            return carry

        lax.fori_loop(0, rows // GROUP, convert, 0, unroll=2)


def gather_kernel(chunk, ask_ref, live_ref, tok_ref, out_ref, raw, table, stage, sems):
    total, width = tok_ref.shape
    peers, block, _ = out_ref.shape
    load_table(tok_ref, raw, table, sems, total // sems.shape[0])
    mask = 2 * total - 1

    def per_peer(d, carry):
        live = jnp.clip(live_ref[d] - chunk * block, 0, block)

        def group(g, carry2):
            base = pl.multiple_of(g * GROUP, GROUP)
            slot = pl.multiple_of((g % 4) * GROUP * SUB, GROUP * SUB)
            for i in range(GROUP):
                row = ask_ref[d, chunk * block + base + i] & mask
                stage[pl.ds(slot + i * SUB, SUB), :] = table[pl.ds(pl.multiple_of(row * SUB, SUB), SUB), :]
            for k in range(width // LANES):
                y = stage[pl.ds(slot + k, GROUP, stride=SUB), :]
                out_ref[d, pl.ds(base, GROUP), k * LANES:(k + 1) * LANES] = y.astype(jnp.bfloat16)
            return carry2

        return lax.fori_loop(0, pl.cdiv(live, GROUP), group, carry)

    lax.fori_loop(0, peers, per_peer, 0)


def ffn_kernel(bound_ref, x_ref, gate_ref, win_ref, wout_ref, out_ref, w1, w2, hidden, sems):
    experts, width, inner = win_ref.shape
    peers, block, _ = x_ref.shape
    tile = hidden.shape[0]
    cut = 512

    def fetch(e, slot):
        return (pltpu.make_async_copy(win_ref.at[e], w1.at[slot], sems.at[0, slot]),
                pltpu.make_async_copy(wout_ref.at[e], w2.at[slot], sems.at[1, slot]))

    for copy in fetch(0, 0):
        copy.start()

    def per_expert(e, carry):
        slot = e % 2
        for copy in fetch(e, slot):
            copy.wait()

        @pl.when(e + 1 < experts)
        def _():
            for copy in fetch(e + 1, 1 - slot):
                copy.start()

        def per_peer(s, carry2):
            lo = bound_ref[s, e]
            hi = bound_ref[s, e + 1]
            first = lo // tile
            last = jnp.where(hi > lo, pl.cdiv(hi, tile), first)

            def per_tile(t, carry3):
                base = pl.multiple_of(t * tile, tile)
                x = x_ref[s, pl.ds(base, tile), :]
                for f in range(inner // cut):
                    pre = jnp.dot(x, w1[slot, :, f * cut:(f + 1) * cut], preferred_element_type=jnp.float32)
                    hidden[:, f * cut:(f + 1) * cut] = jax.nn.gelu(pre, approximate=True).astype(jnp.bfloat16)
                o = jnp.dot(hidden[...], w2[slot], preferred_element_type=jnp.float32)
                p = (gate_ref[s, pl.ds(base, tile), :] * o).astype(jnp.bfloat16).astype(jnp.float32)
                pos = base + lax.broadcasted_iota(jnp.int32, (tile, 1), 0)
                mine = (pos >= lo) & (pos < hi)
                old = out_ref[s, pl.ds(base, tile), :].astype(jnp.float32)
                out_ref[s, pl.ds(base, tile), :] = jnp.where(mine, p, old).astype(jnp.bfloat16)
                return carry3

            return lax.fori_loop(first, last, per_tile, carry2)

        return lax.fori_loop(0, peers, per_peer, carry)

    lax.fori_loop(0, experts, per_expert, 0)


def combine_kernel(ask_ref, live_ref, tok_ref, *refs):
    back_refs = refs[:CHUNKS]
    out_ref, raw, table, stage, rows_buf, out_buf, sems, row_sems, out_sems = refs[CHUNKS:]
    total, width = tok_ref.shape
    peers, block, _ = back_refs[0].shape
    mask = 2 * total - 1

    def fetch(c, d, slot):
        return pltpu.make_async_copy(back_refs[c].at[d], rows_buf.at[slot], row_sems.at[slot])

    fetch(0, 0, 0).start()
    load_table(tok_ref, raw, table, sems, total // sems.shape[0])
    for c in range(CHUNKS):

        def per_peer(d, carry, c=c):
            slot = (c * peers + d) % 2
            fetch(c, d, slot).wait()

            @pl.when(d + 1 < peers)
            def _():
                fetch(c, d + 1, 1 - slot).start()

            if c + 1 < CHUNKS:
                @pl.when(d + 1 == peers)
                def _():
                    fetch(c + 1, 0, 1 - slot).start()

            live = jnp.clip(live_ref[d] - c * block, 0, block)

            def group(g, carry2):
                base = pl.multiple_of(g * GROUP, GROUP)
                for k in range(width // LANES):
                    y = rows_buf[slot, pl.ds(base, GROUP), k * LANES:(k + 1) * LANES]
                    stage[pl.ds(k, GROUP, stride=SUB), :] = y.astype(jnp.float32)
                asks = [ask_ref[d, c * block + base + i] for i in range(GROUP)]
                spots = [pl.ds(pl.multiple_of((a & mask) * SUB, SUB), SUB) for a in asks]
                single = (asks[0] // (mask + 1)) == (asks[GROUP - 1] // (mask + 1))

                @pl.when(single)
                def _():
                    sums = [table[spots[i], :] + stage[i * SUB:(i + 1) * SUB, :] for i in range(GROUP)]
                    for i in range(GROUP):
                        table[spots[i], :] = sums[i]

                @pl.when(jnp.logical_not(single))
                def _():
                    for i in range(GROUP):
                        table[spots[i], :] = table[spots[i], :] + stage[i * SUB:(i + 1) * SUB, :]

                return carry2

            return lax.fori_loop(0, pl.cdiv(live, GROUP), group, carry)

        lax.fori_loop(0, peers, per_peer, 0)

    step = out_buf.shape[1]

    def flush(p, slot):
        return pltpu.make_async_copy(out_buf.at[slot], out_ref.at[pl.ds(p * step, step)], out_sems.at[slot])

    def write(p, carry):
        slot = p % 2

        @pl.when(p >= 2)
        def _():
            flush(p - 2, slot).wait()

        def convert(g, carry2):
            base = pl.multiple_of(g * GROUP, GROUP)
            for k in range(width // LANES):
                y = table[pl.ds((p * step + base) * SUB + k, GROUP, stride=SUB), :]
                out_buf[slot, pl.ds(base, GROUP), k * LANES:(k + 1) * LANES] = y.astype(jnp.bfloat16)
            return carry2

        lax.fori_loop(0, step // GROUP, convert, 0, unroll=2)
        flush(p, slot).start()
        return carry

    n_steps = total // step
    lax.fori_loop(0, n_steps, write, 0)
    for p in range(max(0, n_steps - 2), n_steps):
        flush(p, p % 2).wait()


def solution(mesh):
    peers = mesh.shape["ep"]
    row_spec = P(("dp", "ep"), None)
    expert_spec = P("ep", None, None)
    smem = pl.BlockSpec(memory_space=pltpu.SMEM)
    hbm = pl.BlockSpec(memory_space=pl.ANY)
    vmem = pl.BlockSpec(memory_space=pltpu.VMEM)
    params = pltpu.CompilerParams(vmem_limit_bytes=VMEM_LIMIT)

    def local_layer(tok, sel, gate, win, wout):
        rows, width = tok.shape
        experts, slots = sel.shape
        inner = win.shape[2]
        total = experts * slots
        cap = 2 * total // peers
        block = cap // CHUNKS
        parts = 8

        owner = sel // rows
        lane_e = lax.broadcasted_iota(jnp.int32, (experts, slots), 0)
        key = ((owner * (experts + 1) + lane_e) * rows + sel % rows).reshape(total)
        peer_ids = jnp.arange(peers, dtype=jnp.int32)
        counts = jnp.sum((owner.reshape(1, total) == peer_ids[:, None]).astype(jnp.int32), axis=1)
        fill_end = jnp.cumsum(cap - counts)
        fill_id = jnp.arange(peers * cap - total, dtype=jnp.int32)
        fill_owner = jnp.sum((fill_id[None, :] >= fill_end[:, None]).astype(jnp.int32), axis=0)
        fill_key = (fill_owner * (experts + 1) + experts) * rows + fill_id % rows
        keys, gates = lax.sort(
            (jnp.concatenate([key, fill_key]), jnp.concatenate([gate.reshape(total), jnp.zeros(fill_id.shape, jnp.float32)])),
            num_keys=1, is_stable=False)
        keys = keys.reshape(peers, cap)
        gates = gates.reshape(peers, cap)
        local = keys - peer_ids[:, None] * ((experts + 1) * rows)
        edges = jnp.arange(experts + 1, dtype=jnp.int32) * rows
        bounds = jnp.sum((local[:, None, :] < edges[None, :, None]).astype(jnp.int32), axis=2)
        which = local // rows
        want = which * (2 * rows) + jnp.where(which < experts, local % rows, rows)

        asked = lax.all_to_all(want, "ep", 0, 0, tiled=True)
        live = jnp.sum((asked < experts * 2 * rows).astype(jnp.int32), axis=1)

        def gather(c):
            return pl.pallas_call(
                functools.partial(gather_kernel, c),
                out_shape=jax.ShapeDtypeStruct((peers, block, width), jnp.bfloat16),
                in_specs=[smem, smem, hbm],
                out_specs=vmem,
                scratch_shapes=[
                    pltpu.VMEM((rows, width), jnp.bfloat16),
                    pltpu.VMEM(((rows + 1) * SUB, LANES), jnp.float32),
                    pltpu.VMEM((4 * GROUP * SUB, LANES), jnp.float32),
                    pltpu.SemaphoreType.DMA((parts,)),
                ],
                compiler_params=params,
                cost_estimate=pl.CostEstimate(flops=15_000_000_000, bytes_accessed=3 * rows * width, transcendentals=0),
                name="gather_rows",
            )(asked, live, tok)

        def ffn(c, x):
            cb = jnp.clip(bounds - c * block, 0, block)
            g = gates[:, c * block:(c + 1) * block].reshape(peers, block, 1)
            return pl.pallas_call(
                ffn_kernel,
                out_shape=jax.ShapeDtypeStruct((peers, block, width), jnp.bfloat16),
                in_specs=[smem, vmem, vmem, hbm, hbm],
                out_specs=vmem,
                scratch_shapes=[
                    pltpu.VMEM((2, width, inner), jnp.bfloat16),
                    pltpu.VMEM((2, inner, width), jnp.bfloat16),
                    pltpu.VMEM((min(ROW_TILE, block), inner), jnp.bfloat16),
                    pltpu.SemaphoreType.DMA((2, 2)),
                ],
                compiler_params=params,
                cost_estimate=pl.CostEstimate(
                    flops=4 * total * width * inner // CHUNKS, bytes_accessed=4 * experts * width * inner,
                    transcendentals=total * inner // CHUNKS),
                name="expert_ffn",
            )(cb, x, g, win, wout)

        arrived = [lax.all_to_all(gather(c), "ep", 0, 0, tiled=True) for c in range(CHUNKS)]
        back = [lax.all_to_all(ffn(c, arrived[c]), "ep", 0, 0, tiled=True) for c in range(CHUNKS)]

        step = rows // parts
        return pl.pallas_call(
            combine_kernel,
            out_shape=jax.ShapeDtypeStruct((rows, width), jnp.bfloat16),
            in_specs=[smem, smem, hbm] + [hbm] * CHUNKS,
            out_specs=hbm,
            scratch_shapes=[
                pltpu.VMEM((rows, width), jnp.bfloat16),
                pltpu.VMEM(((rows + 1) * SUB, LANES), jnp.float32),
                pltpu.VMEM((GROUP * SUB, LANES), jnp.float32),
                pltpu.VMEM((2, block, width), jnp.bfloat16),
                pltpu.VMEM((2, step, width), jnp.bfloat16),
                pltpu.SemaphoreType.DMA((parts,)),
                pltpu.SemaphoreType.DMA((2,)),
                pltpu.SemaphoreType.DMA((2,)),
            ],
            compiler_params=params,
            cost_estimate=pl.CostEstimate(flops=40_000_000_000, bytes_accessed=6 * rows * width, transcendentals=0),
            name="combine_rows",
        )(asked, live, tok, *back)

    return jax.shard_map(
        local_layer, mesh=mesh, in_specs=(row_spec, row_spec, row_spec, expert_spec, expert_spec),
        out_specs=row_spec, check_vma=False)
```

```python
import functools

import jax
import jax.numpy as jnp
from jax import lax
from jax.experimental import pallas as pl
from jax.experimental.pallas import tpu as pltpu
from jax.sharding import PartitionSpec as P

LANES = 128
SUB = 8
GROUP = 16
VMEM_LIMIT = 62 * 1024 * 1024
PAIR = 2 * GROUP
SHARES = (5, 3)
ROW_TILE = 256


def load_table(tok_ref, raw, table, sems, rows):
    total, width = tok_ref.shape
    parts = total // rows
    copies = [
        pltpu.make_async_copy(tok_ref.at[pl.ds(p * rows, rows)], raw.at[pl.ds(p * rows, rows)], sems.at[p])
        for p in range(parts)
    ]
    for copy in copies:
        copy.start()
    for p in range(parts):
        copies[p].wait()

        def convert(g, carry):
            base = pl.multiple_of(p * rows + g * GROUP, GROUP)
            for k in range(width // LANES):
                x = raw[pl.ds(base, GROUP), k * LANES:(k + 1) * LANES].astype(jnp.float32)
                table[pl.ds(base * SUB + k, GROUP, stride=SUB), :] = x
            return carry

        lax.fori_loop(0, rows // GROUP, convert, 0, unroll=2)


def gather_kernel(start, cap, ask_ref, live_ref, tok_ref, out_ref, raw, table, stage, sems):
    total, width = tok_ref.shape
    peers, block, _ = out_ref.shape
    load_table(tok_ref, raw, table, sems, total // sems.shape[0])
    mask = 2 * total - 1

    def per_peer(d, carry):
        live = jnp.clip(live_ref[d] - start, 0, block)

        def group(g, carry2):
            base = pl.multiple_of(g * PAIR, PAIR)
            first = d * cap + start + base
            slot = pl.multiple_of((g % 2) * PAIR * SUB, PAIR * SUB)
            for i in range(PAIR):
                row = ask_ref[first + i]
                if i % GROUP == 0:
                    row = row & mask
                stage[pl.ds(slot + i * SUB, SUB), :] = table[pl.ds(pl.multiple_of(row * SUB, SUB), SUB), :]
            for h in range(PAIR // GROUP):
                for k in range(width // LANES):
                    y = stage[pl.ds(slot + h * GROUP * SUB + k, GROUP, stride=SUB), :]
                    out_ref[d, pl.ds(base + h * GROUP, GROUP), k * LANES:(k + 1) * LANES] = y.astype(jnp.bfloat16)
            return carry2

        return lax.fori_loop(0, pl.cdiv(live, PAIR), group, carry)

    lax.fori_loop(0, peers, per_peer, 0)


def ffn_kernel(bound_ref, x_ref, gate_ref, win_ref, wout_ref, out_ref, w1, w2, hidden, sems):
    experts, _, inner = win_ref.shape
    peers, _, _ = x_ref.shape
    tile = hidden.shape[0]
    cut = 512

    def fetch(e, slot):
        return (pltpu.make_async_copy(win_ref.at[e], w1.at[slot], sems.at[0, slot]),
                pltpu.make_async_copy(wout_ref.at[e], w2.at[slot], sems.at[1, slot]))

    for copy in fetch(0, 0):
        copy.start()

    def per_expert(e, carry):
        slot = e % 2
        for copy in fetch(e, slot):
            copy.wait()

        @pl.when(e + 1 < experts)
        def _():
            for copy in fetch(e + 1, 1 - slot):
                copy.start()

        def per_peer(s, carry2):
            lo = bound_ref[s, e]
            hi = bound_ref[s, e + 1]
            first = lo // tile
            last = jnp.where(hi > lo, pl.cdiv(hi, tile), first)

            def per_tile(t, carry3):
                base = pl.multiple_of(t * tile, tile)
                x = x_ref[s, pl.ds(base, tile), :]
                for f in range(inner // cut):
                    pre = jnp.dot(x, w1[slot, :, f * cut:(f + 1) * cut], preferred_element_type=jnp.float32)
                    hidden[:, f * cut:(f + 1) * cut] = jax.nn.gelu(pre, approximate=True).astype(jnp.bfloat16)
                o = jnp.dot(hidden[...], w2[slot], preferred_element_type=jnp.float32)
                p = (gate_ref[s, pl.ds(base, tile), :] * o).astype(jnp.bfloat16).astype(jnp.float32)
                pos = base + lax.broadcasted_iota(jnp.int32, (tile, 1), 0)
                mine = (pos >= lo) & (pos < hi)
                old = out_ref[s, pl.ds(base, tile), :].astype(jnp.float32)
                out_ref[s, pl.ds(base, tile), :] = jnp.where(mine, p, old).astype(jnp.bfloat16)
                return carry3

            return lax.fori_loop(first, last, per_tile, carry2)

        return lax.fori_loop(0, peers, per_peer, carry)

    lax.fori_loop(0, experts, per_expert, 0)


def add_rows(start, cap, ask_ref, live_ref, back_ref, table, stage, rows_buf, row_sems, mask):
    peers, block, width = back_ref.shape

    def fetch(d, slot):
        return pltpu.make_async_copy(back_ref.at[d], rows_buf.at[slot], row_sems.at[slot])

    def per_peer(d, carry):
        slot = d % 2
        fetch(d, slot).wait()

        @pl.when(d + 1 < peers)
        def _():
            fetch(d + 1, 1 - slot).start()

        live = jnp.clip(live_ref[d] - start, 0, block)

        def group(g, carry2):
            base = pl.multiple_of(g * PAIR, PAIR)
            for h in range(PAIR // GROUP):
                for k in range(width // LANES):
                    y = rows_buf[slot, pl.ds(base + h * GROUP, GROUP), k * LANES:(k + 1) * LANES]
                    stage[pl.ds(h * GROUP * SUB + k, GROUP, stride=SUB), :] = y.astype(jnp.float32)
            first = d * cap + start + base
            asks = [ask_ref[first + i] for i in range(PAIR)]
            mixed = asks[0] > mask
            for h in range(1, PAIR // GROUP):
                mixed = jnp.logical_or(mixed, asks[h * GROUP] > mask)
            spots = [pl.ds(pl.multiple_of(((a & mask) if i % GROUP == 0 else a) * SUB, SUB), SUB)
                     for i, a in enumerate(asks)]

            @pl.when(jnp.logical_not(mixed))
            def _():
                for h in range(PAIR // GROUP):
                    ids = range(h * GROUP, (h + 1) * GROUP)
                    sums = [table[spots[i], :] + stage[i * SUB:(i + 1) * SUB, :] for i in ids]
                    for i, v in zip(ids, sums):
                        table[spots[i], :] = v

            @pl.when(mixed)
            def _():
                for i in range(PAIR):
                    table[spots[i], :] = table[spots[i], :] + stage[i * SUB:(i + 1) * SUB, :]

            return carry2

        return lax.fori_loop(0, pl.cdiv(live, PAIR), group, carry)

    return fetch, lambda: lax.fori_loop(0, peers, per_peer, 0)


def first_combine_kernel(start, cap, ask_ref, live_ref, tok_ref, back_ref, sum_ref, raw, table, stage, rows_buf,
                         sems, row_sems, sum_sems):
    total, _ = tok_ref.shape
    fetch, run = add_rows(start, cap, ask_ref, live_ref, back_ref, table, stage, rows_buf, row_sems, 2 * total - 1)
    fetch(0, 0).start()
    load_table(tok_ref, raw, table, sems, total // sems.shape[0])
    run()
    parts = sum_sems.shape[0]
    step = total * SUB // parts
    copies = [pltpu.make_async_copy(table.at[pl.ds(p * step, step)], sum_ref.at[pl.ds(p * step, step)], sum_sems.at[p])
              for p in range(parts)]
    for copy in copies:
        copy.start()
    for copy in copies:
        copy.wait()


def last_combine_kernel(start, cap, ask_ref, live_ref, sum_ref, back_ref, out_ref, table, stage, rows_buf, out_buf,
                        row_sems, sum_sems, out_sems):
    total, width = out_ref.shape
    fetch, run = add_rows(start, cap, ask_ref, live_ref, back_ref, table, stage, rows_buf, row_sems, 2 * total - 1)
    parts = sum_sems.shape[0]
    part = total * SUB // parts
    copies = [pltpu.make_async_copy(sum_ref.at[pl.ds(p * part, part)], table.at[pl.ds(p * part, part)], sum_sems.at[p])
              for p in range(parts)]
    for copy in copies:
        copy.start()
    fetch(0, 0).start()
    for copy in copies:
        copy.wait()
    run()
    step = out_buf.shape[1]

    def flush(p, slot):
        return pltpu.make_async_copy(out_buf.at[slot], out_ref.at[pl.ds(p * step, step)], out_sems.at[slot])

    def write(p, carry):
        slot = p % 2

        @pl.when(p >= 2)
        def _():
            flush(p - 2, slot).wait()

        def convert(g, carry2):
            base = pl.multiple_of(g * GROUP, GROUP)
            for k in range(width // LANES):
                y = table[pl.ds((p * step + base) * SUB + k, GROUP, stride=SUB), :]
                out_buf[slot, pl.ds(base, GROUP), k * LANES:(k + 1) * LANES] = y.astype(jnp.bfloat16)
            return carry2

        lax.fori_loop(0, step // GROUP, convert, 0, unroll=2)
        flush(p, slot).start()
        return carry

    n_steps = total // step
    lax.fori_loop(0, n_steps, write, 0)
    for p in range(max(0, n_steps - 2), n_steps):
        flush(p, p % 2).wait()


def solution(mesh):
    peers = mesh.shape["ep"]
    row_spec = P(("dp", "ep"), None)
    expert_spec = P("ep", None, None)
    smem = pl.BlockSpec(memory_space=pltpu.SMEM)
    hbm = pl.BlockSpec(memory_space=pl.ANY)
    vmem = pl.BlockSpec(memory_space=pltpu.VMEM)
    params = pltpu.CompilerParams(vmem_limit_bytes=VMEM_LIMIT)

    def local_layer(tok, sel, gate, win, wout):
        rows, width = tok.shape
        experts, slots = sel.shape
        inner = win.shape[2]
        total = experts * slots
        cap = 2 * total // peers
        parts = 8
        chunks = []
        for share in SHARES:
            chunks.append((sum(n for _, n in chunks), share * cap // 8))

        owner = sel // rows
        lane_e = lax.broadcasted_iota(jnp.int32, (experts, slots), 0)
        key = ((owner * (experts + 1) + lane_e) * rows + sel % rows).reshape(total)
        peer_ids = jnp.arange(peers, dtype=jnp.int32)
        counts = jnp.sum((owner.reshape(1, total) == peer_ids[:, None]).astype(jnp.int32), axis=1)
        fill_end = jnp.cumsum(cap - counts)
        fill_id = jnp.arange(peers * cap - total, dtype=jnp.int32)
        fill_owner = jnp.sum((fill_id[None, :] >= fill_end[:, None]).astype(jnp.int32), axis=0)
        fill_key = (fill_owner * (experts + 1) + experts) * rows + fill_id % rows
        keys, gates = lax.sort(
            (jnp.concatenate([key, fill_key]), jnp.concatenate([gate.reshape(total), jnp.zeros(fill_id.shape, jnp.float32)])),
            num_keys=1, is_stable=False)
        keys = keys.reshape(peers, cap)
        gates = gates.reshape(peers, cap)
        local = keys - peer_ids[:, None] * ((experts + 1) * rows)
        edges = jnp.arange(experts + 1, dtype=jnp.int32) * rows
        bounds = jnp.sum((local[:, None, :] < edges[None, :, None]).astype(jnp.int32), axis=2)
        which = local // rows
        lane = lax.broadcasted_iota(jnp.int32, (peers, cap), 1)
        mixed = (lane % GROUP == 0) & (which != jnp.roll(which, 1 - GROUP, axis=1))
        want = jnp.where(which < experts, local % rows, rows) + jnp.where(mixed, 2 * rows, 0)

        asked = lax.all_to_all(want, "ep", 0, 0, tiled=True)
        live = jnp.sum((asked & (2 * rows - 1) != rows).astype(jnp.int32), axis=1)
        asked = asked.reshape(peers * cap)

        def gather(c):
            start, block = chunks[c]
            return pl.pallas_call(
                functools.partial(gather_kernel, start, cap),
                out_shape=jax.ShapeDtypeStruct((peers, block, width), jnp.bfloat16),
                in_specs=[smem, smem, hbm],
                out_specs=vmem,
                scratch_shapes=[
                    pltpu.VMEM((rows, width), jnp.bfloat16),
                    pltpu.VMEM(((rows + 1) * SUB, LANES), jnp.float32),
                    pltpu.VMEM((2 * PAIR * SUB, LANES), jnp.float32),
                    pltpu.SemaphoreType.DMA((parts,)),
                ],
                compiler_params=params,
                cost_estimate=pl.CostEstimate(flops=15_000_000_000, bytes_accessed=3 * rows * width, transcendentals=0),
                name="gather_rows",
            )(asked, live, tok)

        def ffn(c, x):
            start, block = chunks[c]
            cb = jnp.clip(bounds - start, 0, block)
            g = gates[:, start:start + block].reshape(peers, block, 1)
            return pl.pallas_call(
                ffn_kernel,
                out_shape=jax.ShapeDtypeStruct((peers, block, width), jnp.bfloat16),
                in_specs=[smem, vmem, vmem, hbm, hbm],
                out_specs=vmem,
                scratch_shapes=[
                    pltpu.VMEM((2, width, inner), jnp.bfloat16),
                    pltpu.VMEM((2, inner, width), jnp.bfloat16),
                    pltpu.VMEM((min(ROW_TILE, block), inner), jnp.bfloat16),
                    pltpu.SemaphoreType.DMA((2, 2)),
                ],
                compiler_params=params,
                cost_estimate=pl.CostEstimate(
                    flops=4 * total * width * inner // len(chunks), bytes_accessed=4 * experts * width * inner,
                    transcendentals=total * inner // len(chunks)),
                name="expert_ffn",
            )(cb, x, g, win, wout)

        def exchange(x):
            return lax.all_to_all(x, "ep", 0, 0, tiled=True)

        sent = [gather(c) for c in range(2)]
        in_a = exchange(sent[0])
        in_b = exchange(sent[1])
        done_a = ffn(0, in_a)
        done_b = ffn(1, in_b)
        back_a = exchange(done_a)
        back_b = exchange(done_b)

        step = rows // parts
        table_shape = pltpu.VMEM(((rows + 1) * SUB, LANES), jnp.float32)
        stage_shape = pltpu.VMEM((PAIR * SUB, LANES), jnp.float32)
        two = pltpu.SemaphoreType.DMA((2,))
        sums = pl.pallas_call(
            functools.partial(first_combine_kernel, chunks[0][0], cap),
            out_shape=jax.ShapeDtypeStruct((rows * SUB, LANES), jnp.float32),
            in_specs=[smem, smem, hbm, hbm],
            out_specs=hbm,
            scratch_shapes=[
                pltpu.VMEM((rows, width), jnp.bfloat16), table_shape, stage_shape,
                pltpu.VMEM((2, chunks[0][1], width), jnp.bfloat16),
                pltpu.SemaphoreType.DMA((parts,)), two, pltpu.SemaphoreType.DMA((parts,)),
            ],
            compiler_params=params,
            cost_estimate=pl.CostEstimate(flops=40_000_000_000, bytes_accessed=6 * rows * width, transcendentals=0),
            name="combine_first",
        )(asked, live, tok, back_a)
        return pl.pallas_call(
            functools.partial(last_combine_kernel, chunks[1][0], cap),
            out_shape=jax.ShapeDtypeStruct((rows, width), jnp.bfloat16),
            in_specs=[smem, smem, hbm, hbm],
            out_specs=hbm,
            scratch_shapes=[
                table_shape, stage_shape, pltpu.VMEM((2, chunks[1][1], width), jnp.bfloat16),
                pltpu.VMEM((2, step, width), jnp.bfloat16), two, pltpu.SemaphoreType.DMA((parts,)), two,
            ],
            compiler_params=params,
            cost_estimate=pl.CostEstimate(flops=20_000_000_000, bytes_accessed=6 * rows * width, transcendentals=0),
            name="combine_last",
        )(asked, live, sums, back_b)

    return jax.shard_map(
        local_layer, mesh=mesh, in_specs=(row_spec, row_spec, row_spec, expert_spec, expert_spec),
        out_specs=row_spec, check_vma=False)
```

```python
import functools

import jax
import jax.numpy as jnp
from jax import lax
from jax.experimental import pallas as pl
from jax.experimental.pallas import tpu as pltpu
from jax.sharding import PartitionSpec as P

LANES = 128
SUB = 8
GROUP = 16
VMEM_LIMIT = 62 * 1024 * 1024
PAIR = 2 * GROUP
SHARES = (5, 3)
ROW_TILE = 256


def load_table(tok_ref, raw, table, sems, rows):
    total, width = tok_ref.shape
    parts = total // rows
    copies = [
        pltpu.make_async_copy(tok_ref.at[pl.ds(p * rows, rows)], raw.at[pl.ds(p * rows, rows)], sems.at[p])
        for p in range(parts)
    ]
    for copy in copies:
        copy.start()
    for p in range(parts):
        copies[p].wait()

        def convert(g, carry):
            base = pl.multiple_of(p * rows + g * GROUP, GROUP)
            for k in range(width // LANES):
                x = raw[pl.ds(base, GROUP), k * LANES:(k + 1) * LANES].astype(jnp.float32)
                table[pl.ds(base * SUB + k, GROUP, stride=SUB), :] = x
            return carry

        lax.fori_loop(0, rows // GROUP, convert, 0, unroll=2)


def gather_kernel(start, cap, dest_ref, ask_ref, live_ref, tok_ref, *refs):
    total, width = tok_ref.shape
    peers = dest_ref.shape[0]
    out_refs = refs[:peers]
    raw, table, stage, out_buf, sems, out_sems = refs[peers:]
    block = out_refs[0].shape[0]
    load_table(tok_ref, raw, table, sems, total // sems.shape[0])
    mask = 2 * total - 1

    def flush(j):
        return pltpu.make_async_copy(out_buf.at[j % 2], out_refs[j], out_sems.at[j % 2])

    for j in range(peers):
        if j >= 2:
            flush(j - 2).wait()
        d = dest_ref[j]
        live = jnp.clip(live_ref[d] - start, 0, block)

        def group(g, carry, j=j, d=d):
            base = pl.multiple_of(g * PAIR, PAIR)
            first = d * cap + start + base
            slot = pl.multiple_of((g % 2) * PAIR * SUB, PAIR * SUB)
            for i in range(PAIR):
                row = ask_ref[first + i]
                if i % GROUP == 0:
                    row = row & mask
                stage[pl.ds(slot + i * SUB, SUB), :] = table[pl.ds(pl.multiple_of(row * SUB, SUB), SUB), :]
            for h in range(PAIR // GROUP):
                for k in range(width // LANES):
                    y = stage[pl.ds(slot + h * GROUP * SUB + k, GROUP, stride=SUB), :]
                    out_buf[j % 2, pl.ds(base + h * GROUP, GROUP), k * LANES:(k + 1) * LANES] = y.astype(jnp.bfloat16)
            return carry

        lax.fori_loop(0, pl.cdiv(live, PAIR), group, 0)
        flush(j).start()
    for j in range(peers - 2, peers):
        flush(j).wait()


def ffn_kernel(bound_ref, gate_ref, win_ref, wout_ref, *refs):
    experts, _, inner = win_ref.shape
    peers = bound_ref.shape[0]
    x_refs, out_refs = refs[:peers], refs[peers:2 * peers]
    xs, outs, w1, w2, hidden, sems, x_sems, out_sems = refs[2 * peers:]
    tile = hidden.shape[0]
    cut = 512

    def fetch(e, slot):
        return (pltpu.make_async_copy(win_ref.at[e], w1.at[slot], sems.at[0, slot]),
                pltpu.make_async_copy(wout_ref.at[e], w2.at[slot], sems.at[1, slot]))

    def bring(s):
        return pltpu.make_async_copy(x_refs[s], xs.at[s], x_sems.at[s])

    def flush(s):
        return pltpu.make_async_copy(outs.at[s], out_refs[s], out_sems.at[s])

    bring(0).start()
    for copy in fetch(0, 0):
        copy.start()
    for s in range(1, peers):
        bring(s).start()

    def per_expert(e, carry):
        slot = e % 2
        for copy in fetch(e, slot):
            copy.wait()

        @pl.when(e + 1 < experts)
        def _():
            for copy in fetch(e + 1, 1 - slot):
                copy.start()

        def per_peer(s, carry2):
            @pl.when(e == 0)
            def _():
                pltpu.make_async_copy(x_refs[0], xs.at[s], x_sems.at[s]).wait()

            lo = bound_ref[s, e]
            hi = bound_ref[s, e + 1]
            first = lo // tile
            last = jnp.where(hi > lo, pl.cdiv(hi, tile), first)

            def per_tile(t, carry3):
                base = pl.multiple_of(t * tile, tile)
                x = xs[s, pl.ds(base, tile), :]
                for f in range(inner // cut):
                    pre = jnp.dot(x, w1[slot, :, f * cut:(f + 1) * cut], preferred_element_type=jnp.float32)
                    hidden[:, f * cut:(f + 1) * cut] = jax.nn.gelu(pre, approximate=True).astype(jnp.bfloat16)
                o = jnp.dot(hidden[...], w2[slot], preferred_element_type=jnp.float32)
                p = (gate_ref[s, pl.ds(base, tile), :] * o).astype(jnp.bfloat16).astype(jnp.float32)
                pos = base + lax.broadcasted_iota(jnp.int32, (tile, 1), 0)
                mine = (pos >= lo) & (pos < hi)
                old = outs[s, pl.ds(base, tile), :].astype(jnp.float32)
                outs[s, pl.ds(base, tile), :] = jnp.where(mine, p, old).astype(jnp.bfloat16)
                return carry3

            lax.fori_loop(first, last, per_tile, 0)
            for j in range(peers):
                @pl.when((e == experts - 1) & (s == j))
                def _():
                    flush(j).start()

            return carry2

        return lax.fori_loop(0, peers, per_peer, carry)

    lax.fori_loop(0, experts, per_expert, 0)
    for s in range(peers):
        flush(s).wait()


def add_rows(start, cap, dest_ref, ask_ref, live_ref, back_refs, table, stage, rows_buf, row_sems, mask):
    peers = len(back_refs)
    block, width = back_refs[0].shape

    def fetch(j, slot):
        return pltpu.make_async_copy(back_refs[j], rows_buf.at[slot], row_sems.at[slot])

    def per_peer(j, carry):
        slot = j % 2
        fetch(0, slot).wait()
        for n in range(1, peers):
            @pl.when(j + 1 == n)
            def _():
                fetch(n, 1 - slot).start()

        d = dest_ref[j]
        live = jnp.clip(live_ref[d] - start, 0, block)

        def group(g, carry2):
            base = pl.multiple_of(g * PAIR, PAIR)
            for h in range(PAIR // GROUP):
                for k in range(width // LANES):
                    y = rows_buf[slot, pl.ds(base + h * GROUP, GROUP), k * LANES:(k + 1) * LANES]
                    stage[pl.ds(h * GROUP * SUB + k, GROUP, stride=SUB), :] = y.astype(jnp.float32)
            first = d * cap + start + base
            asks = [ask_ref[first + i] for i in range(PAIR)]
            mixed = asks[0] > mask
            for h in range(1, PAIR // GROUP):
                mixed = jnp.logical_or(mixed, asks[h * GROUP] > mask)
            spots = [pl.ds(pl.multiple_of(((a & mask) if i % GROUP == 0 else a) * SUB, SUB), SUB)
                     for i, a in enumerate(asks)]

            @pl.when(jnp.logical_not(mixed))
            def _():
                for h in range(PAIR // GROUP):
                    ids = range(h * GROUP, (h + 1) * GROUP)
                    sums = [table[spots[i], :] + stage[i * SUB:(i + 1) * SUB, :] for i in ids]
                    for i, v in zip(ids, sums):
                        table[spots[i], :] = v

            @pl.when(mixed)
            def _():
                for i in range(PAIR):
                    table[spots[i], :] = table[spots[i], :] + stage[i * SUB:(i + 1) * SUB, :]

            return carry2

        return lax.fori_loop(0, pl.cdiv(live, PAIR), group, carry)

    return fetch, lambda: lax.fori_loop(0, peers, per_peer, 0)


def first_combine_kernel(start, cap, dest_ref, ask_ref, live_ref, tok_ref, *refs):
    total, _ = tok_ref.shape
    peers = dest_ref.shape[0]
    back_refs = refs[:peers]
    sum_ref, raw, table, stage, rows_buf, sems, row_sems, sum_sems = refs[peers:]
    fetch, run = add_rows(start, cap, dest_ref, ask_ref, live_ref, back_refs, table, stage, rows_buf, row_sems, 2 * total - 1)
    fetch(0, 0).start()
    load_table(tok_ref, raw, table, sems, total // sems.shape[0])
    run()
    parts = sum_sems.shape[0]
    step = total * SUB // parts
    copies = [pltpu.make_async_copy(table.at[pl.ds(p * step, step)], sum_ref.at[pl.ds(p * step, step)], sum_sems.at[p])
              for p in range(parts)]
    for copy in copies:
        copy.start()
    for copy in copies:
        copy.wait()


def last_combine_kernel(start, cap, dest_ref, ask_ref, live_ref, sum_ref, *refs):
    peers = dest_ref.shape[0]
    back_refs = refs[:peers]
    out_ref, table, stage, rows_buf, out_buf, row_sems, sum_sems, out_sems = refs[peers:]
    total, width = out_ref.shape
    fetch, run = add_rows(start, cap, dest_ref, ask_ref, live_ref, back_refs, table, stage, rows_buf, row_sems, 2 * total - 1)
    parts = sum_sems.shape[0]
    part = total * SUB // parts
    copies = [pltpu.make_async_copy(sum_ref.at[pl.ds(p * part, part)], table.at[pl.ds(p * part, part)], sum_sems.at[p])
              for p in range(parts)]
    for copy in copies:
        copy.start()
    fetch(0, 0).start()
    for copy in copies:
        copy.wait()
    run()
    step = out_buf.shape[1]

    def flush(p, slot):
        return pltpu.make_async_copy(out_buf.at[slot], out_ref.at[pl.ds(p * step, step)], out_sems.at[slot])

    def write(p, carry):
        slot = p % 2

        @pl.when(p >= 2)
        def _():
            flush(p - 2, slot).wait()

        def convert(g, carry2):
            base = pl.multiple_of(g * GROUP, GROUP)
            for k in range(width // LANES):
                y = table[pl.ds((p * step + base) * SUB + k, GROUP, stride=SUB), :]
                out_buf[slot, pl.ds(base, GROUP), k * LANES:(k + 1) * LANES] = y.astype(jnp.bfloat16)
            return carry2

        lax.fori_loop(0, step // GROUP, convert, 0, unroll=2)
        flush(p, slot).start()
        return carry

    n_steps = total // step
    lax.fori_loop(0, n_steps, write, 0)
    for p in range(max(0, n_steps - 2), n_steps):
        flush(p, p % 2).wait()


def solution(mesh):
    peers = mesh.shape["ep"]
    chips = peers // 2
    row_spec = P(("dp", "ep"), None)
    expert_spec = P("ep", None, None)
    smem = pl.BlockSpec(memory_space=pltpu.SMEM)
    hbm = pl.BlockSpec(memory_space=pl.ANY)
    vmem = pl.BlockSpec(memory_space=pltpu.VMEM)
    params = pltpu.CompilerParams(vmem_limit_bytes=VMEM_LIMIT)

    def local_layer(tok, sel, gate, win, wout):
        rows, width = tok.shape
        experts, slots = sel.shape
        inner = win.shape[2]
        total = experts * slots
        cap = 2 * total // peers
        parts = 8
        chunks = []
        for share in SHARES:
            chunks.append((sum(n for _, n in chunks), share * cap // 8))

        owner = sel // rows
        lane_e = lax.broadcasted_iota(jnp.int32, (experts, slots), 0)
        key = ((owner * (experts + 1) + lane_e) * rows + sel % rows).reshape(total)
        peer_ids = jnp.arange(peers, dtype=jnp.int32)
        counts = jnp.sum((owner.reshape(1, total) == peer_ids[:, None]).astype(jnp.int32), axis=1)
        fill_end = jnp.cumsum(cap - counts)
        fill_id = jnp.arange(peers * cap - total, dtype=jnp.int32)
        fill_owner = jnp.sum((fill_id[None, :] >= fill_end[:, None]).astype(jnp.int32), axis=0)
        fill_key = (fill_owner * (experts + 1) + experts) * rows + fill_id % rows
        keys, gates = lax.sort(
            (jnp.concatenate([key, fill_key]), jnp.concatenate([gate.reshape(total), jnp.zeros(fill_id.shape, jnp.float32)])),
            num_keys=1, is_stable=False)
        keys = keys.reshape(peers, cap)
        gates = gates.reshape(peers, cap)
        local = keys - peer_ids[:, None] * ((experts + 1) * rows)
        edges = jnp.arange(experts + 1, dtype=jnp.int32) * rows
        bounds = jnp.sum((local[:, None, :] < edges[None, :, None]).astype(jnp.int32), axis=2)
        which = local // rows
        lane = lax.broadcasted_iota(jnp.int32, (peers, cap), 1)
        mixed = (lane % GROUP == 0) & (which != jnp.roll(which, 1 - GROUP, axis=1))
        want = jnp.where(which < experts, local % rows, rows) + jnp.where(mixed, 2 * rows, 0)

        asked = lax.all_to_all(want, "ep", 0, 0, tiled=True)
        live = jnp.sum((asked & (2 * rows - 1) != rows).astype(jnp.int32), axis=1)
        asked = asked.reshape(peers * cap)

        hops = [(0, 0), (1, 0), (1, 1), (chips - 1, 0), (chips - 1, 1), (0, 1)]
        hops += [(n, flip) for n in range(2, chips - 1) for flip in (0, 1)]
        me = lax.axis_index("ep")
        dests = jnp.stack([(me // 2 + n) % chips * 2 + (me % 2 + f) % 2 for n, f in hops])
        sources = jnp.stack([(me // 2 + chips - n) % chips * 2 + (me % 2 + f) % 2 for n, f in hops])
        onehot = (sources[:, None] == peer_ids[None, :]).astype(jnp.int32)

        def exchange(xs, forward):
            ys = []
            for x, (n, f) in zip(xs, hops):
                there = [(i // 2 + n) % chips * 2 + (i % 2 + f) % 2 for i in range(peers)]
                pairs = [(i, j) if forward else (j, i) for i, j in enumerate(there)]
                ys.append(x if (n, f) == (0, 0) else lax.ppermute(x, "ep", pairs))
            return ys

        def blocks(c):
            return [jax.ShapeDtypeStruct((chunks[c][1], width), jnp.bfloat16)] * peers

        def gather(c):
            start, block = chunks[c]
            return pl.pallas_call(
                functools.partial(gather_kernel, start, cap),
                out_shape=blocks(c),
                in_specs=[smem, smem, smem, hbm],
                out_specs=[hbm] * peers,
                scratch_shapes=[
                    pltpu.VMEM((rows, width), jnp.bfloat16),
                    pltpu.VMEM(((rows + 1) * SUB, LANES), jnp.float32),
                    pltpu.VMEM((2 * PAIR * SUB, LANES), jnp.float32),
                    pltpu.VMEM((2, block, width), jnp.bfloat16),
                    pltpu.SemaphoreType.DMA((parts,)),
                    pltpu.SemaphoreType.DMA((2,)),
                ],
                compiler_params=params,
                cost_estimate=pl.CostEstimate(flops=15_000_000_000, bytes_accessed=3 * rows * width, transcendentals=0),
                name="gather_rows",
            )(dests, asked, live, tok)

        def ffn(c, x):
            start, block = chunks[c]
            cb = jnp.clip(hop_bounds - start, 0, block)
            g = hop_gates[:, start:start + block].reshape(peers, block, 1)
            return pl.pallas_call(
                ffn_kernel,
                out_shape=blocks(c),
                in_specs=[smem, vmem, hbm, hbm] + [hbm] * peers,
                out_specs=[hbm] * peers,
                scratch_shapes=[
                    pltpu.VMEM((peers, block, width), jnp.bfloat16),
                    pltpu.VMEM((peers, block, width), jnp.bfloat16),
                    pltpu.VMEM((2, width, inner), jnp.bfloat16),
                    pltpu.VMEM((2, inner, width), jnp.bfloat16),
                    pltpu.VMEM((min(ROW_TILE, block), inner), jnp.bfloat16),
                    pltpu.SemaphoreType.DMA((2, 2)),
                    pltpu.SemaphoreType.DMA((peers,)),
                    pltpu.SemaphoreType.DMA((peers,)),
                ],
                compiler_params=params,
                cost_estimate=pl.CostEstimate(
                    flops=4 * total * width * inner // len(chunks), bytes_accessed=4 * experts * width * inner,
                    transcendentals=total * inner // len(chunks)),
                name="expert_ffn",
            )(cb, g, win, wout, *x)

        hop_bounds = jnp.sum(onehot[:, :, None] * bounds[None], axis=1)
        hop_gates = jnp.sum(jnp.where(onehot[:, :, None] > 0, gates[None], 0.0), axis=1)

        sent = [gather(c) for c in range(2)]
        in_a = exchange(sent[0], True)
        in_b = exchange(sent[1], True)
        done_a = ffn(0, in_a)
        done_b = ffn(1, in_b)
        back_a = exchange(done_a, False)
        back_b = exchange(done_b, False)

        step = rows // parts
        table_shape = pltpu.VMEM(((rows + 1) * SUB, LANES), jnp.float32)
        stage_shape = pltpu.VMEM((PAIR * SUB, LANES), jnp.float32)
        two = pltpu.SemaphoreType.DMA((2,))
        sums = pl.pallas_call(
            functools.partial(first_combine_kernel, chunks[0][0], cap),
            out_shape=jax.ShapeDtypeStruct((rows * SUB, LANES), jnp.float32),
            in_specs=[smem, smem, smem, hbm] + [hbm] * peers,
            out_specs=hbm,
            scratch_shapes=[
                pltpu.VMEM((rows, width), jnp.bfloat16), table_shape, stage_shape,
                pltpu.VMEM((2, chunks[0][1], width), jnp.bfloat16),
                pltpu.SemaphoreType.DMA((parts,)), two, pltpu.SemaphoreType.DMA((parts,)),
            ],
            compiler_params=params,
            cost_estimate=pl.CostEstimate(flops=40_000_000_000, bytes_accessed=6 * rows * width, transcendentals=0),
            name="combine_first",
        )(dests, asked, live, tok, *back_a)
        return pl.pallas_call(
            functools.partial(last_combine_kernel, chunks[1][0], cap),
            out_shape=jax.ShapeDtypeStruct((rows, width), jnp.bfloat16),
            in_specs=[smem, smem, smem, hbm] + [hbm] * peers,
            out_specs=hbm,
            scratch_shapes=[
                table_shape, stage_shape, pltpu.VMEM((2, chunks[1][1], width), jnp.bfloat16),
                pltpu.VMEM((2, step, width), jnp.bfloat16), two, pltpu.SemaphoreType.DMA((parts,)), two,
            ],
            compiler_params=params,
            cost_estimate=pl.CostEstimate(flops=20_000_000_000, bytes_accessed=6 * rows * width, transcendentals=0),
            name="combine_last",
        )(dests, asked, live, sums, *back_b)

    return jax.shard_map(
        local_layer, mesh=mesh, in_specs=(row_spec, row_spec, row_spec, expert_spec, expert_spec),
        out_specs=row_spec, check_vma=False)
```

```python
import functools

import jax
import jax.numpy as jnp
from jax import lax
from jax.experimental import pallas as pl
from jax.experimental.pallas import tpu as pltpu
from jax.sharding import PartitionSpec as P

LANES = 128
SUB = 8
GROUP = 16
VMEM_LIMIT = 62 * 1024 * 1024
LEAN_LIMIT = 63 * 1024 * 1024 // 2
PAIR = 2 * GROUP
SHARES = (1, 5, 2)
ROW_TILE = 256


def load_table(tok_ref, raw, table, sems, rows):
    total, width = tok_ref.shape
    parts = total // rows
    copies = [
        pltpu.make_async_copy(tok_ref.at[pl.ds(p * rows, rows)], raw.at[pl.ds(p * rows, rows)], sems.at[p])
        for p in range(parts)
    ]
    for copy in copies:
        copy.start()
    for p in range(parts):
        copies[p].wait()

        def convert(g, carry):
            base = pl.multiple_of(p * rows + g * GROUP, GROUP)
            for k in range(width // LANES):
                x = raw[pl.ds(base, GROUP), k * LANES:(k + 1) * LANES].astype(jnp.float32)
                table[pl.ds(base * SUB + k, GROUP, stride=SUB), :] = x
            return carry

        lax.fori_loop(0, rows // GROUP, convert, 0, unroll=2)


def gather_kernel(start, cap, dest_ref, ask_ref, live_ref, tok_ref, *refs):
    total, width = tok_ref.shape
    peers = dest_ref.shape[0]
    out_refs = refs[:peers]
    raw, table, stage, out_buf, sems, out_sems = refs[peers:]
    block = out_refs[0].shape[0]
    load_table(tok_ref, raw, table, sems, total // sems.shape[0])
    mask = 2 * total - 1

    def flush(j):
        return pltpu.make_async_copy(out_buf.at[j % 2], out_refs[j], out_sems.at[j % 2])

    for j in range(peers):
        if j >= 2:
            flush(j - 2).wait()
        d = dest_ref[j]
        live = jnp.clip(live_ref[d] - start, 0, block)

        def group(g, carry, j=j, d=d):
            base = pl.multiple_of(g * PAIR, PAIR)
            first = d * cap + start + base
            slot = pl.multiple_of((g % 2) * PAIR * SUB, PAIR * SUB)
            for i in range(PAIR):
                row = ask_ref[first + i]
                if i % GROUP == 0:
                    row = row & mask
                stage[pl.ds(slot + i * SUB, SUB), :] = table[pl.ds(pl.multiple_of(row * SUB, SUB), SUB), :]
            for h in range(PAIR // GROUP):
                for k in range(width // LANES):
                    y = stage[pl.ds(slot + h * GROUP * SUB + k, GROUP, stride=SUB), :]
                    out_buf[j % 2, pl.ds(base + h * GROUP, GROUP), k * LANES:(k + 1) * LANES] = y.astype(jnp.bfloat16)
            return carry

        lax.fori_loop(0, pl.cdiv(live, PAIR), group, 0)
        flush(j).start()
    for j in range(peers - 2, peers):
        flush(j).wait()


def ffn_kernel(bound_ref, gate_ref, win_ref, wout_ref, *refs):
    experts, width, inner = win_ref.shape
    peers = bound_ref.shape[0]
    x_refs, out_refs = refs[:peers], refs[peers:2 * peers]
    xs, outs, w1, w2, hidden, sems, x_sems, out_sems = refs[2 * peers:]
    tile = hidden.shape[0]
    cut = 512

    def fetch(e, slot):
        return (pltpu.make_async_copy(win_ref.at[e], w1.at[slot], sems.at[0, slot]),
                pltpu.make_async_copy(wout_ref.at[e], w2.at[slot], sems.at[1, slot]))

    def bring(s):
        return pltpu.make_async_copy(x_refs[s], xs.at[s], x_sems.at[s])

    def flush(s):
        return pltpu.make_async_copy(outs.at[s], out_refs[s], out_sems.at[s])

    bring(0).start()
    for copy in fetch(0, 0):
        copy.start()
    for s in range(1, peers):
        bring(s).start()

    def per_expert(e, carry):
        slot = e % 2
        for copy in fetch(e, slot):
            copy.wait()

        @pl.when(e + 1 < experts)
        def _():
            for copy in fetch(e + 1, 1 - slot):
                copy.start()

        def per_peer(s, carry2):
            @pl.when(e == 0)
            def _():
                pltpu.make_async_copy(x_refs[0], xs.at[s], x_sems.at[s]).wait()

            lo = bound_ref[s, e]
            hi = bound_ref[s, e + 1]
            first = lo // tile
            last = jnp.where(hi > lo, pl.cdiv(hi, tile), first)

            def per_tile(t, carry3):
                base = pl.multiple_of(t * tile, tile)
                x = xs[s, pl.ds(base, tile), :]
                for f in range(inner // cut):
                    pre = jnp.dot(x, w1[slot, :, f * cut:(f + 1) * cut], preferred_element_type=jnp.float32)
                    hidden[:, f * cut:(f + 1) * cut] = jax.nn.gelu(pre, approximate=True).astype(jnp.bfloat16)
                o = jnp.dot(hidden[...], w2[slot], preferred_element_type=jnp.float32)
                p = (gate_ref[s, pl.ds(base, tile), :] * o).astype(jnp.bfloat16).astype(jnp.float32)
                pos = base + lax.broadcasted_iota(jnp.int32, (tile, 1), 0)
                mine = (pos >= lo) & (pos < hi)
                old = outs[s, pl.ds(base, tile), :].astype(jnp.float32)
                outs[s, pl.ds(base, tile), :] = jnp.where(mine, p, old).astype(jnp.bfloat16)
                return carry3

            lax.fori_loop(first, last, per_tile, 0)
            for j in range(peers):
                @pl.when((e == experts - 1) & (s == j))
                def _():
                    flush(j).start()

            return carry2

        return lax.fori_loop(0, peers, per_peer, carry)

    lax.fori_loop(0, experts, per_expert, 0)
    for s in range(peers):
        flush(s).wait()


def add_rows(start, cap, dest_ref, ask_ref, live_ref, back_refs, table, stage, rows_buf, row_sems, mask):
    peers = len(back_refs)
    block, width = back_refs[0].shape

    def fetch(j, slot):
        return pltpu.make_async_copy(back_refs[j], rows_buf.at[slot, pl.ds(0, block)], row_sems.at[slot])

    def per_peer(j, carry):
        slot = j % 2
        fetch(0, slot).wait()
        for n in range(1, peers):
            @pl.when(j + 1 == n)
            def _():
                fetch(n, 1 - slot).start()

        d = dest_ref[j]
        live = jnp.clip(live_ref[d] - start, 0, block)

        def group(g, carry2):
            base = pl.multiple_of(g * PAIR, PAIR)
            for h in range(PAIR // GROUP):
                for k in range(width // LANES):
                    y = rows_buf[slot, pl.ds(base + h * GROUP, GROUP), k * LANES:(k + 1) * LANES]
                    stage[pl.ds(h * GROUP * SUB + k, GROUP, stride=SUB), :] = y.astype(jnp.float32)
            first = d * cap + start + base
            asks = [ask_ref[first + i] for i in range(PAIR)]
            mixed = asks[0] > mask
            for h in range(1, PAIR // GROUP):
                mixed = jnp.logical_or(mixed, asks[h * GROUP] > mask)
            spots = [pl.ds(pl.multiple_of(((a & mask) if i % GROUP == 0 else a) * SUB, SUB), SUB)
                     for i, a in enumerate(asks)]

            @pl.when(jnp.logical_not(mixed))
            def _():
                for h in range(PAIR // GROUP):
                    ids = range(h * GROUP, (h + 1) * GROUP)
                    sums = [table[spots[i], :] + stage[i * SUB:(i + 1) * SUB, :] for i in ids]
                    for i, v in zip(ids, sums):
                        table[spots[i], :] = v

            @pl.when(mixed)
            def _():
                for i in range(PAIR):
                    table[spots[i], :] = table[spots[i], :] + stage[i * SUB:(i + 1) * SUB, :]

            return carry2

        return lax.fori_loop(0, pl.cdiv(live, PAIR), group, carry)

    return fetch, lambda: lax.fori_loop(0, peers, per_peer, 0)


def first_combine_kernel(chunks, cap, dest_ref, ask_ref, live_ref, tok_ref, *refs):
    total, _ = tok_ref.shape
    peers = dest_ref.shape[0]
    count = peers * len(chunks)
    back_refs = refs[:count]
    table, raw, stage, rows_buf, sems, row_sems = refs[count:]
    runs = [add_rows(start, cap, dest_ref, ask_ref, live_ref, back_refs[n * peers:(n + 1) * peers], table, stage,
                     rows_buf, row_sems, 2 * total - 1) for n, (start, _) in enumerate(chunks)]
    runs[0][0](0, 0).start()
    load_table(tok_ref, raw, table, sems, total // sems.shape[0])
    for n, (fetch, run) in enumerate(runs):
        if n > 0:
            fetch(0, 0).start()
        run()


def last_combine_kernel(start, cap, dest_ref, ask_ref, live_ref, table, *refs):
    peers = dest_ref.shape[0]
    back_refs = refs[:peers]
    out_ref, stage, rows_buf, out_buf, row_sems, out_sems = refs[peers:]
    total, width = out_ref.shape
    fetch, run = add_rows(start, cap, dest_ref, ask_ref, live_ref, back_refs, table, stage, rows_buf, row_sems, 2 * total - 1)
    fetch(0, 0).start()
    run()
    step = out_buf.shape[1]

    def flush(p, slot):
        return pltpu.make_async_copy(out_buf.at[slot], out_ref.at[pl.ds(p * step, step)], out_sems.at[slot])

    def write(p, carry):
        slot = p % 2

        @pl.when(p >= 2)
        def _():
            flush(p - 2, slot).wait()

        def convert(g, carry2):
            base = pl.multiple_of(g * GROUP, GROUP)
            for k in range(width // LANES):
                y = table[pl.ds((p * step + base) * SUB + k, GROUP, stride=SUB), :]
                out_buf[slot, pl.ds(base, GROUP), k * LANES:(k + 1) * LANES] = y.astype(jnp.bfloat16)
            return carry2

        lax.fori_loop(0, step // GROUP, convert, 0, unroll=2)
        flush(p, slot).start()
        return carry

    n_steps = total // step
    lax.fori_loop(0, n_steps, write, 0)
    for p in range(max(0, n_steps - 2), n_steps):
        flush(p, p % 2).wait()


def solution(mesh):
    peers = mesh.shape["ep"]
    chips = peers // 2
    row_spec = P(("dp", "ep"), None)
    expert_spec = P("ep", None, None)
    smem = pl.BlockSpec(memory_space=pltpu.SMEM)
    hbm = pl.BlockSpec(memory_space=pl.ANY)
    vmem = pl.BlockSpec(memory_space=pltpu.VMEM)
    params = pltpu.CompilerParams(vmem_limit_bytes=VMEM_LIMIT)
    lean = pltpu.CompilerParams(vmem_limit_bytes=LEAN_LIMIT)

    def local_layer(tok, sel, gate, win, wout):
        rows, width = tok.shape
        experts, slots = sel.shape
        inner = win.shape[2]
        total = experts * slots
        cap = 2 * total // peers
        parts = 8
        chunks = []
        for share in SHARES:
            chunks.append((sum(n for _, n in chunks), share * cap // 8))

        owner = sel // rows
        lane_e = lax.broadcasted_iota(jnp.int32, (experts, slots), 0)
        key = ((owner * (experts + 1) + lane_e) * rows + sel % rows).reshape(total)
        peer_ids = jnp.arange(peers, dtype=jnp.int32)
        counts = jnp.sum((owner.reshape(1, total) == peer_ids[:, None]).astype(jnp.int32), axis=1)
        fill_end = jnp.cumsum(cap - counts)
        fill_id = jnp.arange(peers * cap - total, dtype=jnp.int32)
        fill_owner = jnp.sum((fill_id[None, :] >= fill_end[:, None]).astype(jnp.int32), axis=0)
        fill_key = (fill_owner * (experts + 1) + experts) * rows + fill_id % rows
        keys, gates = lax.sort(
            (jnp.concatenate([key, fill_key]), jnp.concatenate([gate.reshape(total), jnp.zeros(fill_id.shape, jnp.float32)])),
            num_keys=1, is_stable=False)
        keys = keys.reshape(peers, cap)
        gates = gates.reshape(peers, cap)
        local = keys - peer_ids[:, None] * ((experts + 1) * rows)
        edges = jnp.arange(experts + 1, dtype=jnp.int32) * rows
        bounds = jnp.sum((local[:, None, :] < edges[None, :, None]).astype(jnp.int32), axis=2)
        which = local // rows
        lane = lax.broadcasted_iota(jnp.int32, (peers, cap), 1)
        mixed = (lane % GROUP == 0) & (which != jnp.roll(which, 1 - GROUP, axis=1))
        want = jnp.where(which < experts, local % rows, rows) + jnp.where(mixed, 2 * rows, 0)

        asked = lax.all_to_all(want, "ep", 0, 0, tiled=True)
        live = jnp.sum((asked & (2 * rows - 1) != rows).astype(jnp.int32), axis=1)
        asked = asked.reshape(peers * cap)

        hops = [(0, 0), (1, 0), (1, 1), (chips - 1, 0), (chips - 1, 1), (0, 1)]
        hops += [(n, flip) for n in range(2, chips - 1) for flip in (0, 1)]
        me = lax.axis_index("ep")
        dests = jnp.stack([(me // 2 + n) % chips * 2 + (me % 2 + f) % 2 for n, f in hops])
        sources = jnp.stack([(me // 2 + chips - n) % chips * 2 + (me % 2 + f) % 2 for n, f in hops])
        onehot = (sources[:, None] == peer_ids[None, :]).astype(jnp.int32)

        def exchange(xs, forward):
            ys = []
            for x, (n, f) in zip(xs, hops):
                there = [(i // 2 + n) % chips * 2 + (i % 2 + f) % 2 for i in range(peers)]
                pairs = [(i, j) if forward else (j, i) for i, j in enumerate(there)]
                ys.append(x if (n, f) == (0, 0) else pltpu.with_memory_space_constraint(lax.ppermute(x, "ep", pairs), pltpu.HBM))
            return ys

        def blocks(c):
            return [pltpu.HBM((chunks[c][1], width), jnp.bfloat16)] * peers

        table_type = pltpu.VMEM(((rows + 1) * SUB, LANES), jnp.float32)
        raw_type = pltpu.VMEM((rows, width), jnp.bfloat16)
        stage_type = pltpu.VMEM((2 * PAIR * SUB, LANES), jnp.float32)
        two = pltpu.SemaphoreType.DMA((2,))

        def gather(c, after):
            start, block = chunks[c]
            turn = lax.optimization_barrier((live, after))[0]
            return pl.pallas_call(
                functools.partial(gather_kernel, start, cap),
                out_shape=blocks(c),
                in_specs=[smem, smem, smem, hbm],
                out_specs=[hbm] * peers,
                scratch_shapes=[
                    raw_type, table_type, stage_type, pltpu.VMEM((2, block, width), jnp.bfloat16),
                    pltpu.SemaphoreType.DMA((parts,)), two,
                ],
                compiler_params=params,
                cost_estimate=pl.CostEstimate(flops=15_000_000_000, bytes_accessed=3 * rows * width, transcendentals=0),
                name="gather_rows",
            )(dests, asked, turn, tok)

        def ffn(c, x):
            start, block = chunks[c]
            cb = jnp.clip(hop_bounds - start, 0, block)
            g = hop_gates[:, start:start + block].reshape(peers, block, 1)
            return pl.pallas_call(
                ffn_kernel,
                out_shape=blocks(c),
                in_specs=[smem, vmem, hbm, hbm] + [hbm] * peers,
                out_specs=[hbm] * peers,
                scratch_shapes=[
                    pltpu.VMEM((peers, block, width), jnp.bfloat16),
                    pltpu.VMEM((peers, block, width), jnp.bfloat16),
                    pltpu.VMEM((2, width, inner), jnp.bfloat16),
                    pltpu.VMEM((2, inner, width), jnp.bfloat16),
                    pltpu.VMEM((min(ROW_TILE, block), inner), jnp.bfloat16),
                    pltpu.SemaphoreType.DMA((2, 2)),
                    pltpu.SemaphoreType.DMA((peers,)),
                    pltpu.SemaphoreType.DMA((peers,)),
                ],
                compiler_params=params,
                cost_estimate=pl.CostEstimate(
                    flops=4 * total * width * inner // len(chunks), bytes_accessed=4 * experts * width * inner,
                    transcendentals=total * inner // len(chunks)),
                name="expert_ffn",
            )(cb, g, win, wout, *x)

        hop_bounds = jnp.sum(onehot[:, :, None] * bounds[None], axis=1)
        hop_gates = jnp.sum(jnp.where(onehot[:, :, None] > 0, gates[None], 0.0), axis=1)

        sent = []
        for c in range(len(chunks)):
            sent.append(gather(c, sent[-1][0] if sent else tok))
        inputs = [exchange(x, True) for x in sent]
        done = [ffn(c, x) for c, x in enumerate(inputs)]
        back = [exchange(x, False) for x in done]

        early, last = chunks[:-1], chunks[-1]
        step = rows // parts
        sums = pl.pallas_call(
            functools.partial(first_combine_kernel, early, cap),
            out_shape=table_type,
            in_specs=[smem, smem, smem, hbm] + [hbm] * (peers * len(early)),
            out_specs=vmem,
            scratch_shapes=[
                raw_type, stage_type, pltpu.VMEM((2, max(n for _, n in early), width), jnp.bfloat16),
                pltpu.SemaphoreType.DMA((parts,)), two,
            ],
            compiler_params=lean,
            cost_estimate=pl.CostEstimate(flops=40_000_000_000, bytes_accessed=6 * rows * width, transcendentals=0),
            name="combine_first",
        )(dests, asked, live, tok, *[x for xs in back[:-1] for x in xs])
        return pl.pallas_call(
            functools.partial(last_combine_kernel, last[0], cap),
            out_shape=jax.ShapeDtypeStruct((rows, width), jnp.bfloat16),
            in_specs=[smem, smem, smem, vmem] + [hbm] * peers,
            out_specs=hbm,
            scratch_shapes=[
                stage_type, pltpu.VMEM((2, last[1], width), jnp.bfloat16),
                pltpu.VMEM((2, step, width), jnp.bfloat16), two, two,
            ],
            compiler_params=lean,
            cost_estimate=pl.CostEstimate(flops=20_000_000_000, bytes_accessed=6 * rows * width, transcendentals=0),
            name="combine_last",
        )(dests, asked, live, pltpu.with_memory_space_constraint(sums, pltpu.VMEM), *back[-1])

    return jax.shard_map(
        local_layer, mesh=mesh, in_specs=(row_spec, row_spec, row_spec, expert_spec, expert_spec),
        out_specs=row_spec, check_vma=False)
```

```python
import functools

import jax
import jax.numpy as jnp
from jax import lax
from jax.experimental import pallas as pl
from jax.experimental.pallas import tpu as pltpu
from jax.sharding import PartitionSpec as P

LANES = 128
SUB = 8
GROUP = 16
VMEM_LIMIT = 62 * 1024 * 1024
LEAN_LIMIT = 63 * 1024 * 1024 // 2
PAIR = 2 * GROUP
SHARES = (1, 5, 2)
ROW_TILE = 256


def load_table(tok_ref, raw, table, sems, rows):
    total, width = tok_ref.shape
    parts = total // rows
    copies = [
        pltpu.make_async_copy(tok_ref.at[pl.ds(p * rows, rows)], raw.at[pl.ds(p * rows, rows)], sems.at[p])
        for p in range(parts)
    ]
    for copy in copies:
        copy.start()
    for p in range(parts):
        copies[p].wait()

        def convert(g, carry):
            base = pl.multiple_of(p * rows + g * GROUP, GROUP)
            for k in range(width // LANES):
                x = raw[pl.ds(base, GROUP), k * LANES:(k + 1) * LANES].astype(jnp.float32)
                table[pl.ds(base * SUB + k, GROUP, stride=SUB), :] = x
            return carry

        lax.fori_loop(0, rows // GROUP, convert, 0, unroll=2)


def table_kernel(tok_ref, table, raw, sems):
    load_table(tok_ref, raw, table, sems, tok_ref.shape[0] // sems.shape[0])


def pick_rows(start, ask_refs, table, out_refs, stage, out_buf, out_sems):
    peers = len(ask_refs)
    block, width = out_refs[0].shape
    cap = ask_refs[0].shape[0] - LANES
    total = table.shape[0] // SUB - 1
    mask = 2 * total - 1

    def flush(j):
        return pltpu.make_async_copy(out_buf.at[j % 2], out_refs[j], out_sems.at[j % 2])

    for j, ask_ref in enumerate(ask_refs):
        if j >= 2:
            flush(j - 2).wait()
        live = jnp.clip(ask_ref[cap] - start, 0, block)

        def group(g, carry, j=j, ask_ref=ask_ref):
            base = pl.multiple_of(g * PAIR, PAIR)
            first = start + base
            slot = pl.multiple_of((g % 2) * PAIR * SUB, PAIR * SUB)
            for i in range(PAIR):
                row = ask_ref[first + i]
                if i % GROUP == 0:
                    row = row & mask
                stage[pl.ds(slot + i * SUB, SUB), :] = table[pl.ds(pl.multiple_of(row * SUB, SUB), SUB), :]
            for h in range(PAIR // GROUP):
                for k in range(width // LANES):
                    y = stage[pl.ds(slot + h * GROUP * SUB + k, GROUP, stride=SUB), :]
                    out_buf[j % 2, pl.ds(base + h * GROUP, GROUP), k * LANES:(k + 1) * LANES] = y.astype(jnp.bfloat16)
            return carry

        lax.fori_loop(0, pl.cdiv(live, PAIR), group, 0)
        flush(j).start()
    for j in range(peers - 2, peers):
        flush(j).wait()


def first_gather_kernel(start, peers, *refs):
    pick_rows(start, refs[:peers], refs[peers], refs[peers + 1:2 * peers + 1], *refs[2 * peers + 1:])


def gather_kernel(start, peers, *refs):
    tok_ref = refs[peers]
    raw, table, stage, out_buf, sems, out_sems = refs[2 * peers + 1:]
    load_table(tok_ref, raw, table, sems, tok_ref.shape[0] // sems.shape[0])
    pick_rows(start, refs[:peers], table, refs[peers + 1:2 * peers + 1], stage, out_buf, out_sems)


def ffn_kernel(bound_ref, gate_ref, win_ref, wout_ref, *refs):
    experts, width, inner = win_ref.shape
    peers = bound_ref.shape[0]
    x_refs, out_refs = refs[:peers], refs[peers:2 * peers]
    xs, outs, w1, w2, hidden, sems, x_sems, out_sems = refs[2 * peers:]
    tile = hidden.shape[0]
    cut = 512

    def fetch(e, slot):
        return (pltpu.make_async_copy(win_ref.at[e], w1.at[slot], sems.at[0, slot]),
                pltpu.make_async_copy(wout_ref.at[e], w2.at[slot], sems.at[1, slot]))

    def bring(s):
        return pltpu.make_async_copy(x_refs[s], xs.at[s], x_sems.at[s])

    def flush(s):
        return pltpu.make_async_copy(outs.at[s], out_refs[s], out_sems.at[s])

    bring(0).start()
    for copy in fetch(0, 0):
        copy.start()
    for s in range(1, peers):
        bring(s).start()

    def per_expert(e, carry):
        slot = e % 2
        for copy in fetch(e, slot):
            copy.wait()

        @pl.when(e + 1 < experts)
        def _():
            for copy in fetch(e + 1, 1 - slot):
                copy.start()

        def per_peer(s, carry2):
            @pl.when(e == 0)
            def _():
                pltpu.make_async_copy(x_refs[0], xs.at[s], x_sems.at[s]).wait()

            lo = bound_ref[s, e]
            hi = bound_ref[s, e + 1]
            first = lo // tile
            last = jnp.where(hi > lo, pl.cdiv(hi, tile), first)

            def per_tile(t, carry3):
                base = pl.multiple_of(t * tile, tile)
                x = xs[s, pl.ds(base, tile), :]
                for f in range(inner // cut):
                    pre = jnp.dot(x, w1[slot, :, f * cut:(f + 1) * cut], preferred_element_type=jnp.float32)
                    hidden[:, f * cut:(f + 1) * cut] = jax.nn.gelu(pre, approximate=True).astype(jnp.bfloat16)
                o = jnp.dot(hidden[...], w2[slot], preferred_element_type=jnp.float32)
                p = (gate_ref[s, pl.ds(base, tile), :] * o).astype(jnp.bfloat16).astype(jnp.float32)
                pos = base + lax.broadcasted_iota(jnp.int32, (tile, 1), 0)
                mine = (pos >= lo) & (pos < hi)
                old = outs[s, pl.ds(base, tile), :].astype(jnp.float32)
                outs[s, pl.ds(base, tile), :] = jnp.where(mine, p, old).astype(jnp.bfloat16)
                return carry3

            lax.fori_loop(first, last, per_tile, 0)
            for j in range(peers):
                @pl.when((e == experts - 1) & (s == j))
                def _():
                    flush(j).start()

            return carry2

        return lax.fori_loop(0, peers, per_peer, carry)

    lax.fori_loop(0, experts, per_expert, 0)
    for s in range(peers):
        flush(s).wait()


def add_rows(start, ask_refs, back_refs, table, stage, rows_buf, row_sems):
    peers = len(back_refs)
    block, width = back_refs[0].shape
    cap = ask_refs[0].shape[0] - LANES
    mask = 2 * (table.shape[0] // SUB - 1) - 1

    def fetch(j):
        return pltpu.make_async_copy(back_refs[j], rows_buf.at[j % 2, pl.ds(0, block)], row_sems.at[j % 2])

    def per_peer(j):
        ask_ref = ask_refs[j]
        slot = j % 2
        fetch(j).wait()
        if j + 1 < peers:
            fetch(j + 1).start()
        live = jnp.clip(ask_ref[cap] - start, 0, block)

        def group(g, carry2):
            base = pl.multiple_of(g * PAIR, PAIR)
            for h in range(PAIR // GROUP):
                for k in range(width // LANES):
                    y = rows_buf[slot, pl.ds(base + h * GROUP, GROUP), k * LANES:(k + 1) * LANES]
                    stage[pl.ds(h * GROUP * SUB + k, GROUP, stride=SUB), :] = y.astype(jnp.float32)
            first = start + base
            asks = [ask_ref[first + i] for i in range(PAIR)]
            mixed = asks[0] > mask
            for h in range(1, PAIR // GROUP):
                mixed = jnp.logical_or(mixed, asks[h * GROUP] > mask)
            spots = [pl.ds(pl.multiple_of(((a & mask) if i % GROUP == 0 else a) * SUB, SUB), SUB)
                     for i, a in enumerate(asks)]

            @pl.when(jnp.logical_not(mixed))
            def _():
                for h in range(PAIR // GROUP):
                    ids = range(h * GROUP, (h + 1) * GROUP)
                    sums = [table[spots[i], :] + stage[i * SUB:(i + 1) * SUB, :] for i in ids]
                    for i, v in zip(ids, sums):
                        table[spots[i], :] = v

            @pl.when(mixed)
            def _():
                for i in range(PAIR):
                    table[spots[i], :] = table[spots[i], :] + stage[i * SUB:(i + 1) * SUB, :]

            return carry2

        lax.fori_loop(0, pl.cdiv(live, PAIR), group, 0)

    def run():
        for j in range(peers):
            per_peer(j)

    return fetch, run


def first_combine_kernel(chunks, peers, *refs):
    ask_refs, tok_ref = refs[:peers], refs[peers]
    total, _ = tok_ref.shape
    count = peers * len(chunks)
    back_refs = refs[peers + 1:peers + 1 + count]
    table, raw, stage, rows_buf, sems, row_sems = refs[peers + 1 + count:]
    runs = [add_rows(start, ask_refs, back_refs[n * peers:(n + 1) * peers], table, stage, rows_buf, row_sems)
            for n, (start, _) in enumerate(chunks)]
    runs[0][0](0).start()
    load_table(tok_ref, raw, table, sems, total // sems.shape[0])
    for n, (fetch, run) in enumerate(runs):
        if n > 0:
            fetch(0).start()
        run()


def last_combine_kernel(start, peers, *refs):
    ask_refs, table, back_refs = refs[:peers], refs[peers], refs[peers + 1:2 * peers + 1]
    out_ref, stage, rows_buf, out_buf, row_sems, out_sems = refs[2 * peers + 1:]
    total, width = out_ref.shape
    fetch, run = add_rows(start, ask_refs, back_refs, table, stage, rows_buf, row_sems)
    fetch(0).start()
    run()
    step = out_buf.shape[1]

    def flush(p, slot):
        return pltpu.make_async_copy(out_buf.at[slot], out_ref.at[pl.ds(p * step, step)], out_sems.at[slot])

    def write(p, carry):
        slot = p % 2

        @pl.when(p >= 2)
        def _():
            flush(p - 2, slot).wait()

        def convert(g, carry2):
            base = pl.multiple_of(g * GROUP, GROUP)
            for k in range(width // LANES):
                y = table[pl.ds((p * step + base) * SUB + k, GROUP, stride=SUB), :]
                out_buf[slot, pl.ds(base, GROUP), k * LANES:(k + 1) * LANES] = y.astype(jnp.bfloat16)
            return carry2

        lax.fori_loop(0, step // GROUP, convert, 0, unroll=2)
        flush(p, slot).start()
        return carry

    n_steps = total // step
    lax.fori_loop(0, n_steps, write, 0)
    for p in range(max(0, n_steps - 2), n_steps):
        flush(p, p % 2).wait()


def solution(mesh):
    peers = mesh.shape["ep"]
    chips = peers // 2
    row_spec = P(("dp", "ep"), None)
    expert_spec = P("ep", None, None)
    smem = pl.BlockSpec(memory_space=pltpu.SMEM)
    hbm = pl.BlockSpec(memory_space=pl.ANY)
    vmem = pl.BlockSpec(memory_space=pltpu.VMEM)
    params = pltpu.CompilerParams(vmem_limit_bytes=VMEM_LIMIT)
    lean = pltpu.CompilerParams(vmem_limit_bytes=LEAN_LIMIT)

    def local_layer(tok, sel, gate, win, wout):
        rows, width = tok.shape
        experts, slots = sel.shape
        inner = win.shape[2]
        total = experts * slots
        cap = 2 * total // peers
        parts = 8
        chunks = []
        for share in SHARES:
            chunks.append((sum(n for _, n in chunks), share * cap // 8))

        hops = [(n, f) for n in range(chips) for f in range(2)]
        me = lax.axis_index("ep")
        device = sel // rows
        owner = (me // 2 + chips - device // 2) % chips * 2 + (me + device) % 2

        lane_e = lax.broadcasted_iota(jnp.int32, (experts, slots), 0)
        key = ((owner * (experts + 1) + lane_e) * rows + sel % rows).reshape(total)
        peer_ids = jnp.arange(peers, dtype=jnp.int32)
        counts = jnp.sum((owner.reshape(1, total) == peer_ids[:, None]).astype(jnp.int32), axis=1)
        fill_end = jnp.cumsum(cap - counts)
        fill_id = jnp.arange(peers * cap - total, dtype=jnp.int32)
        fill_owner = jnp.sum((fill_id[None, :] >= fill_end[:, None]).astype(jnp.int32), axis=0)
        fill_key = (fill_owner * (experts + 1) + experts) * rows + fill_id % rows
        keys, gates = lax.sort(
            (jnp.concatenate([key, fill_key]), jnp.concatenate([gate.reshape(total), jnp.zeros(fill_id.shape, jnp.float32)])),
            num_keys=1, is_stable=False)
        keys = keys.reshape(peers, cap)
        local = keys - peer_ids[:, None] * ((experts + 1) * rows)
        edges = jnp.arange(experts + 1, dtype=jnp.int32) * rows
        bounds = jnp.sum((local[:, None, :] < edges[None, :, None]).astype(jnp.int32), axis=2)
        which = local // rows
        lane = lax.broadcasted_iota(jnp.int32, (peers, cap), 1)
        mixed = (lane % GROUP == 0) & (which != jnp.roll(which, 1 - GROUP, axis=1))
        want = jnp.where(which < experts, local % rows, rows) + jnp.where(mixed, 2 * rows, 0)

        want = jnp.concatenate([want, jnp.broadcast_to(bounds[:, experts:], (peers, LANES))], axis=1)

        def exchange(xs, forward, pin=True):
            ys = []
            for x, (n, f) in zip(xs, hops):
                there = [(i // 2 + n) % chips * 2 + (i % 2 + f) % 2 for i in range(peers)]
                pairs = [(i, j) if forward else (j, i) for i, j in enumerate(there)]
                if (n, f) != (0, 0):
                    x = lax.ppermute(x, "ep", pairs)
                    x = pltpu.with_memory_space_constraint(x, pltpu.HBM) if pin else x
                ys.append(x)
            return ys

        asked = exchange([want[j] for j in range(peers)], False, pin=False)

        def blocks(c):
            return [pltpu.HBM((chunks[c][1], width), jnp.bfloat16)] * peers

        table_type = pltpu.VMEM(((rows + 1) * SUB, LANES), jnp.float32)
        raw_type = pltpu.VMEM((rows, width), jnp.bfloat16)
        stage_type = pltpu.VMEM((2 * PAIR * SUB, LANES), jnp.float32)
        two = pltpu.SemaphoreType.DMA((2,))

        table = pl.pallas_call(
            table_kernel,
            out_shape=table_type,
            in_specs=[hbm],
            out_specs=vmem,
            scratch_shapes=[raw_type, pltpu.SemaphoreType.DMA((parts,))],
            compiler_params=lean,
            cost_estimate=pl.CostEstimate(flops=10_000_000_000, bytes_accessed=2 * rows * width, transcendentals=0),
            name="row_table",
        )(tok)

        def gather(c, after):
            start, block = chunks[c]
            first = after is None
            turn = asked if first else lax.optimization_barrier((*asked, after))[:peers]
            buffers = [stage_type, pltpu.VMEM((2, block, width), jnp.bfloat16)]
            if not first:
                buffers = [raw_type, table_type] + buffers + [pltpu.SemaphoreType.DMA((parts,))]
            return pl.pallas_call(
                functools.partial(first_gather_kernel if first else gather_kernel, start, peers),
                out_shape=blocks(c),
                in_specs=[smem] * peers + [vmem if first else hbm],
                out_specs=[hbm] * peers,
                scratch_shapes=buffers + [two],
                compiler_params=lean if first else params,
                cost_estimate=pl.CostEstimate(flops=15_000_000_000, bytes_accessed=3 * rows * width, transcendentals=0),
                name="gather_rows",
            )(*turn, pltpu.with_memory_space_constraint(table, pltpu.VMEM) if first else tok)

        def ffn(c, x):
            start, block = chunks[c]
            cb = jnp.clip(bounds - start, 0, block)
            g = gates[:, start:start + block].reshape(peers, block, 1)
            return pl.pallas_call(
                ffn_kernel,
                out_shape=blocks(c),
                in_specs=[smem, vmem, hbm, hbm] + [hbm] * peers,
                out_specs=[hbm] * peers,
                scratch_shapes=[
                    pltpu.VMEM((peers, block, width), jnp.bfloat16),
                    pltpu.VMEM((peers, block, width), jnp.bfloat16),
                    pltpu.VMEM((2, width, inner), jnp.bfloat16),
                    pltpu.VMEM((2, inner, width), jnp.bfloat16),
                    pltpu.VMEM((min(ROW_TILE, block), inner), jnp.bfloat16),
                    pltpu.SemaphoreType.DMA((2, 2)),
                    pltpu.SemaphoreType.DMA((peers,)),
                    pltpu.SemaphoreType.DMA((peers,)),
                ],
                compiler_params=params,
                cost_estimate=pl.CostEstimate(
                    flops=4 * total * width * inner // len(chunks), bytes_accessed=4 * experts * width * inner,
                    transcendentals=total * inner // len(chunks)),
                name="expert_ffn",
            )(cb, g, win, wout, *x)

        sent = []
        for c in range(len(chunks)):
            sent.append(gather(c, sent[-1][0] if sent else None))
        bounds, gates = lax.optimization_barrier((bounds, gates, sent[1][0]))[:2]
        gates = gates.reshape(peers, cap)
        inputs = [exchange(x, True) for x in sent]
        done = [ffn(c, x) for c, x in enumerate(inputs)]
        back = [exchange(x, False) for x in done]

        early, last = chunks[:-1], chunks[-1]
        step = rows // parts
        sums = pl.pallas_call(
            functools.partial(first_combine_kernel, early, peers),
            out_shape=table_type,
            in_specs=[smem] * peers + [hbm] + [hbm] * (peers * len(early)),
            out_specs=vmem,
            scratch_shapes=[
                raw_type, stage_type, pltpu.VMEM((2, max(n for _, n in early), width), jnp.bfloat16),
                pltpu.SemaphoreType.DMA((parts,)), two,
            ],
            compiler_params=lean,
            cost_estimate=pl.CostEstimate(flops=40_000_000_000, bytes_accessed=6 * rows * width, transcendentals=0),
            name="combine_first",
        )(*asked, tok, *[x for xs in back[:-1] for x in xs])
        return pl.pallas_call(
            functools.partial(last_combine_kernel, last[0], peers),
            out_shape=jax.ShapeDtypeStruct((rows, width), jnp.bfloat16),
            in_specs=[smem] * peers + [vmem] + [hbm] * peers,
            out_specs=hbm,
            scratch_shapes=[
                stage_type, pltpu.VMEM((2, last[1], width), jnp.bfloat16),
                pltpu.VMEM((2, step, width), jnp.bfloat16), two, two,
            ],
            compiler_params=lean,
            cost_estimate=pl.CostEstimate(flops=20_000_000_000, bytes_accessed=6 * rows * width, transcendentals=0),
            name="combine_last",
        )(*asked, pltpu.with_memory_space_constraint(sums, pltpu.VMEM), *back[-1])

    return jax.shard_map(
        local_layer, mesh=mesh, in_specs=(row_spec, row_spec, row_spec, expert_spec, expert_spec),
        out_specs=row_spec, check_vma=False)
```

```python
import functools

import jax
import jax.numpy as jnp
from jax import lax
from jax.experimental import pallas as pl
from jax.experimental.pallas import tpu as pltpu
from jax.sharding import PartitionSpec as P

LANES = 128
SUB = 8
GROUP = 16
VMEM_LIMIT = 62 * 1024 * 1024
LEAN_LIMIT = 63 * 1024 * 1024 // 2
PAIR = 2 * GROUP
SHARES = (1, 5, 2)
ROW_TILE = 256


def load_table(tok_ref, raw, table, sems, rows):
    total, width = tok_ref.shape
    parts = total // rows
    copies = [
        pltpu.make_async_copy(tok_ref.at[pl.ds(p * rows, rows)], raw.at[pl.ds(p * rows, rows)], sems.at[p])
        for p in range(parts)
    ]
    for copy in copies:
        copy.start()
    for p in range(parts):
        copies[p].wait()

        def convert(g, carry):
            base = pl.multiple_of(p * rows + g * GROUP, GROUP)
            for k in range(width // LANES):
                x = raw[pl.ds(base, GROUP), k * LANES:(k + 1) * LANES].astype(jnp.float32)
                table[pl.ds(base * SUB + k, GROUP, stride=SUB), :] = x
            return carry

        lax.fori_loop(0, rows // GROUP, convert, 0, unroll=2)


def table_kernel(tok_ref, table, raw, sems):
    load_table(tok_ref, raw, table, sems, tok_ref.shape[0] // sems.shape[0])


def pick_rows(start, ask_refs, table, out_refs, stage, out_buf, out_sems):
    peers = len(ask_refs)
    block, width = out_refs[0].shape
    cap = ask_refs[0].shape[0] - LANES
    total = table.shape[0] // SUB - 1
    mask = 2 * total - 1

    def flush(j):
        return pltpu.make_async_copy(out_buf.at[j % 2], out_refs[j], out_sems.at[j % 2])

    for j, ask_ref in enumerate(ask_refs):
        if j >= 2:
            flush(j - 2).wait()
        live = jnp.clip(ask_ref[cap] - start, 0, block)

        def group(g, carry, j=j, ask_ref=ask_ref):
            base = pl.multiple_of(g * PAIR, PAIR)
            first = start + base
            slot = pl.multiple_of((g % 2) * PAIR * SUB, PAIR * SUB)
            for i in range(PAIR):
                row = ask_ref[first + i]
                if i % GROUP == 0:
                    row = row & mask
                stage[pl.ds(slot + i * SUB, SUB), :] = table[pl.ds(pl.multiple_of(row * SUB, SUB), SUB), :]
            for h in range(PAIR // GROUP):
                for k in range(width // LANES):
                    y = stage[pl.ds(slot + h * GROUP * SUB + k, GROUP, stride=SUB), :]
                    out_buf[j % 2, pl.ds(base + h * GROUP, GROUP), k * LANES:(k + 1) * LANES] = y.astype(jnp.bfloat16)
            return carry

        lax.fori_loop(0, pl.cdiv(live, PAIR), group, 0)
        flush(j).start()
    for j in range(peers - 2, peers):
        flush(j).wait()


def first_gather_kernel(start, peers, *refs):
    pick_rows(start, refs[:peers], refs[peers], refs[peers + 1:2 * peers + 1], *refs[2 * peers + 1:])


def gather_kernel(start, peers, *refs):
    tok_ref = refs[peers]
    raw, table, stage, out_buf, sems, out_sems = refs[2 * peers + 1:]
    load_table(tok_ref, raw, table, sems, tok_ref.shape[0] // sems.shape[0])
    pick_rows(start, refs[:peers], table, refs[peers + 1:2 * peers + 1], stage, out_buf, out_sems)


def ffn_kernel(bound_ref, gate_ref, win_ref, wout_ref, *refs):
    experts, width, inner = win_ref.shape
    peers = bound_ref.shape[0]
    x_refs, out_refs = refs[:peers], refs[peers:2 * peers]
    xs, outs, w1, w2, hidden, sems, x_sems, out_sems = refs[2 * peers:]
    tile = hidden.shape[0]
    cut = 512

    def fetch(e, slot):
        return (pltpu.make_async_copy(win_ref.at[e], w1.at[slot], sems.at[0, slot]),
                pltpu.make_async_copy(wout_ref.at[e], w2.at[slot], sems.at[1, slot]))

    def bring(s):
        return pltpu.make_async_copy(x_refs[s], xs.at[s], x_sems.at[s])

    def flush(s):
        return pltpu.make_async_copy(outs.at[s], out_refs[s], out_sems.at[s])

    bring(0).start()
    for copy in fetch(0, 0):
        copy.start()
    for s in range(1, peers):
        bring(s).start()

    def per_expert(e, carry):
        slot = e % 2
        for copy in fetch(e, slot):
            copy.wait()

        @pl.when(e + 1 < experts)
        def _():
            for copy in fetch(e + 1, 1 - slot):
                copy.start()

        def per_peer(s, carry2):
            @pl.when(e == 0)
            def _():
                pltpu.make_async_copy(x_refs[0], xs.at[s], x_sems.at[s]).wait()

            lo = bound_ref[s, e]
            hi = bound_ref[s, e + 1]
            first = lo // tile
            last = jnp.where(hi > lo, pl.cdiv(hi, tile), first)

            def per_tile(t, carry3):
                base = pl.multiple_of(t * tile, tile)
                x = xs[s, pl.ds(base, tile), :]
                for f in range(inner // cut):
                    pre = jnp.dot(x, w1[slot, :, f * cut:(f + 1) * cut], preferred_element_type=jnp.float32)
                    hidden[:, f * cut:(f + 1) * cut] = jax.nn.gelu(pre, approximate=True).astype(jnp.bfloat16)
                o = jnp.dot(hidden[...], w2[slot], preferred_element_type=jnp.float32)
                p = (gate_ref[s, pl.ds(base, tile), :] * o).astype(jnp.bfloat16).astype(jnp.float32)
                pos = base + lax.broadcasted_iota(jnp.int32, (tile, 1), 0)
                mine = (pos >= lo) & (pos < hi)
                old = outs[s, pl.ds(base, tile), :].astype(jnp.float32)
                outs[s, pl.ds(base, tile), :] = jnp.where(mine, p, old).astype(jnp.bfloat16)
                return carry3

            lax.fori_loop(first, last, per_tile, 0)
            for j in range(peers):
                @pl.when((e == experts - 1) & (s == j))
                def _():
                    flush(j).start()

            return carry2

        return lax.fori_loop(0, peers, per_peer, carry)

    lax.fori_loop(0, experts, per_expert, 0)
    for s in range(peers):
        flush(s).wait()


def add_rows(start, ask_refs, back_refs, table, stage, rows_buf, row_sems):
    peers = len(back_refs)
    block, width = back_refs[0].shape
    cap = ask_refs[0].shape[0] - LANES
    mask = 2 * (table.shape[0] // SUB - 1) - 1

    def fetch(j):
        return pltpu.make_async_copy(back_refs[j], rows_buf.at[j % 2, pl.ds(0, block)], row_sems.at[j % 2])

    def per_peer(j):
        ask_ref = ask_refs[j]
        slot = j % 2
        fetch(j).wait()
        if j + 1 < peers:
            fetch(j + 1).start()
        live = jnp.clip(ask_ref[cap] - start, 0, block)

        def group(g, carry2):
            base = pl.multiple_of(g * PAIR, PAIR)
            for h in range(PAIR // GROUP):
                for k in range(width // LANES):
                    y = rows_buf[slot, pl.ds(base + h * GROUP, GROUP), k * LANES:(k + 1) * LANES]
                    stage[pl.ds(h * GROUP * SUB + k, GROUP, stride=SUB), :] = y.astype(jnp.float32)
            first = start + base
            asks = [ask_ref[first + i] for i in range(PAIR)]
            mixed = asks[0] > mask
            for h in range(1, PAIR // GROUP):
                mixed = jnp.logical_or(mixed, asks[h * GROUP] > mask)
            spots = [pl.ds(pl.multiple_of(((a & mask) if i % GROUP == 0 else a) * SUB, SUB), SUB)
                     for i, a in enumerate(asks)]

            @pl.when(jnp.logical_not(mixed))
            def _():
                for h in range(PAIR // GROUP):
                    ids = range(h * GROUP, (h + 1) * GROUP)
                    sums = [table[spots[i], :] + stage[i * SUB:(i + 1) * SUB, :] for i in ids]
                    for i, v in zip(ids, sums):
                        table[spots[i], :] = v

            @pl.when(mixed)
            def _():
                for i in range(PAIR):
                    table[spots[i], :] = table[spots[i], :] + stage[i * SUB:(i + 1) * SUB, :]

            return carry2

        lax.fori_loop(0, pl.cdiv(live, PAIR), group, 0)

    def run():
        for j in range(peers):
            per_peer(j)

    return fetch, run


def first_combine_kernel(chunks, peers, *refs):
    ask_refs, tok_ref = refs[:peers], refs[peers]
    total, _ = tok_ref.shape
    count = peers * len(chunks)
    back_refs = refs[peers + 1:peers + 1 + count]
    table, raw, stage, rows_buf, sems, row_sems = refs[peers + 1 + count:]
    runs = [add_rows(start, ask_refs, back_refs[n * peers:(n + 1) * peers], table, stage, rows_buf, row_sems)
            for n, (start, _) in enumerate(chunks)]
    runs[0][0](0).start()
    load_table(tok_ref, raw, table, sems, total // sems.shape[0])
    for n, (fetch, run) in enumerate(runs):
        if n > 0:
            fetch(0).start()
        run()


def last_combine_kernel(start, peers, *refs):
    ask_refs, table, back_refs = refs[:peers], refs[peers], refs[peers + 1:2 * peers + 1]
    out_ref, stage, rows_buf, out_buf, row_sems, out_sems = refs[2 * peers + 1:]
    total, width = out_ref.shape
    fetch, run = add_rows(start, ask_refs, back_refs, table, stage, rows_buf, row_sems)
    fetch(0).start()
    run()
    step = out_buf.shape[1]

    def flush(p, slot):
        return pltpu.make_async_copy(out_buf.at[slot], out_ref.at[pl.ds(p * step, step)], out_sems.at[slot])

    def write(p, carry):
        slot = p % 2

        @pl.when(p >= 2)
        def _():
            flush(p - 2, slot).wait()

        def convert(g, carry2):
            base = pl.multiple_of(g * GROUP, GROUP)
            for k in range(width // LANES):
                y = table[pl.ds((p * step + base) * SUB + k, GROUP, stride=SUB), :]
                out_buf[slot, pl.ds(base, GROUP), k * LANES:(k + 1) * LANES] = y.astype(jnp.bfloat16)
            return carry2

        lax.fori_loop(0, step // GROUP, convert, 0, unroll=2)
        flush(p, slot).start()
        return carry

    n_steps = total // step
    lax.fori_loop(0, n_steps, write, 0)
    for p in range(max(0, n_steps - 2), n_steps):
        flush(p, p % 2).wait()


def solution(mesh):
    peers = mesh.shape["ep"]
    chips = peers // 2
    row_spec = P(("dp", "ep"), None)
    expert_spec = P("ep", None, None)
    smem = pl.BlockSpec(memory_space=pltpu.SMEM)
    hbm = pl.BlockSpec(memory_space=pl.ANY)
    vmem = pl.BlockSpec(memory_space=pltpu.VMEM)
    params = pltpu.CompilerParams(vmem_limit_bytes=VMEM_LIMIT)
    lean = pltpu.CompilerParams(vmem_limit_bytes=LEAN_LIMIT)

    def local_layer(tok, sel, gate, win, wout):
        rows, width = tok.shape
        experts, slots = sel.shape
        inner = win.shape[2]
        total = experts * slots
        cap = 2 * total // peers
        parts = 8
        chunks = []
        for share in SHARES:
            chunks.append((sum(n for _, n in chunks), share * cap // 8))

        hops = [(n, f) for n in range(chips) for f in range(2)]
        me = lax.axis_index("ep")
        device = sel // rows
        owner = (me // 2 + chips - device // 2) % chips * 2 + (me + device) % 2

        lane_e = lax.broadcasted_iota(jnp.int32, (experts, slots), 0)
        key = ((owner * (experts + 1) + lane_e) * rows + sel % rows).reshape(total)
        peer_ids = jnp.arange(peers, dtype=jnp.int32)
        counts = jnp.sum((owner.reshape(1, total) == peer_ids[:, None]).astype(jnp.int32), axis=1)
        fill_end = jnp.cumsum(cap - counts)
        fill_id = jnp.arange(peers * cap - total, dtype=jnp.int32)
        fill_owner = jnp.sum((fill_id[None, :] >= fill_end[:, None]).astype(jnp.int32), axis=0)
        fill_key = (fill_owner * (experts + 1) + experts) * rows + fill_id % rows
        keys, gates = lax.sort(
            (jnp.concatenate([key, fill_key]), jnp.concatenate([gate.reshape(total), jnp.zeros(fill_id.shape, jnp.float32)])),
            num_keys=1, is_stable=False)
        keys = keys.reshape(peers, cap)
        local = keys - peer_ids[:, None] * ((experts + 1) * rows)
        edges = jnp.arange(experts + 1, dtype=jnp.int32) * rows
        bounds = jnp.sum((local[:, None, :] < edges[None, :, None]).astype(jnp.int32), axis=2)
        which = local // rows
        lane = lax.broadcasted_iota(jnp.int32, (peers, cap), 1)
        mixed = (lane % GROUP == 0) & (which != jnp.roll(which, 1 - GROUP, axis=1))
        want = jnp.where(which < experts, local % rows, rows) + jnp.where(mixed, 2 * rows, 0)

        want = jnp.concatenate([want, jnp.broadcast_to(bounds[:, experts:], (peers, LANES))], axis=1)

        def exchange(xs, forward, pin=True):
            ys = []
            for x, (n, f) in zip(xs, hops):
                there = [(i // 2 + n) % chips * 2 + (i % 2 + f) % 2 for i in range(peers)]
                pairs = [(i, j) if forward else (j, i) for i, j in enumerate(there)]
                if (n, f) != (0, 0):
                    x = lax.ppermute(x, "ep", pairs)
                    x = pltpu.with_memory_space_constraint(x, pltpu.HBM) if pin else x
                ys.append(x)
            return ys

        asked = exchange([want[j] for j in range(peers)], False, pin=False)

        def blocks(c):
            return [pltpu.HBM((chunks[c][1], width), jnp.bfloat16)] * peers

        table_type = pltpu.VMEM(((rows + 1) * SUB, LANES), jnp.float32)
        raw_type = pltpu.VMEM((rows, width), jnp.bfloat16)
        stage_type = pltpu.VMEM((2 * PAIR * SUB, LANES), jnp.float32)
        two = pltpu.SemaphoreType.DMA((2,))

        table = pl.pallas_call(
            table_kernel,
            out_shape=table_type,
            in_specs=[hbm],
            out_specs=vmem,
            scratch_shapes=[raw_type, pltpu.SemaphoreType.DMA((parts,))],
            compiler_params=lean,
            cost_estimate=pl.CostEstimate(flops=10_000_000_000, bytes_accessed=2 * rows * width, transcendentals=0),
            name="row_table",
        )(tok)

        def gather(c, after):
            start, block = chunks[c]
            first = after is None
            turn = asked if first else lax.optimization_barrier((*asked, after))[:peers]
            buffers = [stage_type, pltpu.VMEM((2, block, width), jnp.bfloat16)]
            if not first:
                buffers = [raw_type, table_type] + buffers + [pltpu.SemaphoreType.DMA((parts,))]
            return pl.pallas_call(
                functools.partial(first_gather_kernel if first else gather_kernel, start, peers),
                out_shape=blocks(c),
                in_specs=[smem] * peers + [vmem if first else hbm],
                out_specs=[hbm] * peers,
                scratch_shapes=buffers + [two],
                compiler_params=lean if first else params,
                cost_estimate=pl.CostEstimate(flops=15_000_000_000, bytes_accessed=3 * rows * width, transcendentals=0),
                name="gather_rows",
            )(*turn, pltpu.with_memory_space_constraint(table, pltpu.VMEM) if first else tok)

        def ffn(c, x):
            start, block = chunks[c]
            cb = jnp.clip(bounds - start, 0, block)
            g = gates[:, start:start + block].reshape(peers, block, 1)
            return pl.pallas_call(
                ffn_kernel,
                out_shape=blocks(c),
                in_specs=[smem, vmem, hbm, hbm] + [hbm] * peers,
                out_specs=[hbm] * peers,
                scratch_shapes=[
                    pltpu.VMEM((peers, block, width), jnp.bfloat16),
                    pltpu.VMEM((peers, block, width), jnp.bfloat16),
                    pltpu.VMEM((2, width, inner), jnp.bfloat16),
                    pltpu.VMEM((2, inner, width), jnp.bfloat16),
                    pltpu.VMEM((min(ROW_TILE, block), inner), jnp.bfloat16),
                    pltpu.SemaphoreType.DMA((2, 2)),
                    pltpu.SemaphoreType.DMA((peers,)),
                    pltpu.SemaphoreType.DMA((peers,)),
                ],
                compiler_params=params,
                cost_estimate=pl.CostEstimate(
                    flops=4 * total * width * inner // len(chunks), bytes_accessed=4 * experts * width * inner,
                    transcendentals=total * inner // len(chunks)),
                name="expert_ffn",
            )(cb, g, win, wout, *x)

        sent = []
        for c in range(len(chunks)):
            sent.append(gather(c, sent[-1][0] if sent else None))
        inputs = [exchange(x, True) for x in sent]
        bounds, gates = lax.optimization_barrier((bounds, gates, inputs[0][-1]))[:2]
        gates = gates.reshape(peers, cap)
        done = [ffn(c, x) for c, x in enumerate(inputs)]
        back = [exchange(x, False) for x in done]

        early, last = chunks[:-1], chunks[-1]
        step = rows // parts
        sums = pl.pallas_call(
            functools.partial(first_combine_kernel, early, peers),
            out_shape=table_type,
            in_specs=[smem] * peers + [hbm] + [hbm] * (peers * len(early)),
            out_specs=vmem,
            scratch_shapes=[
                raw_type, stage_type, pltpu.VMEM((2, max(n for _, n in early), width), jnp.bfloat16),
                pltpu.SemaphoreType.DMA((parts,)), two,
            ],
            compiler_params=lean,
            cost_estimate=pl.CostEstimate(flops=40_000_000_000, bytes_accessed=6 * rows * width, transcendentals=0),
            name="combine_first",
        )(*asked, tok, *[x for xs in back[:-1] for x in xs])
        return pl.pallas_call(
            functools.partial(last_combine_kernel, last[0], peers),
            out_shape=jax.ShapeDtypeStruct((rows, width), jnp.bfloat16),
            in_specs=[smem] * peers + [vmem] + [hbm] * peers,
            out_specs=hbm,
            scratch_shapes=[
                stage_type, pltpu.VMEM((2, last[1], width), jnp.bfloat16),
                pltpu.VMEM((2, step, width), jnp.bfloat16), two, two,
            ],
            compiler_params=lean,
            cost_estimate=pl.CostEstimate(flops=20_000_000_000, bytes_accessed=6 * rows * width, transcendentals=0),
            name="combine_last",
        )(*asked, pltpu.with_memory_space_constraint(sums, pltpu.VMEM), *back[-1])

    return jax.shard_map(
        local_layer, mesh=mesh, in_specs=(row_spec, row_spec, row_spec, expert_spec, expert_spec),
        out_specs=row_spec, check_vma=False)
```

```python
import functools

import jax
import jax.numpy as jnp
from jax import lax
from jax.experimental import pallas as pl
from jax.experimental.pallas import tpu as pltpu
from jax.sharding import PartitionSpec as P

LANES = 128
SUB = 8
GROUP = 16
VMEM_LIMIT = 62 * 1024 * 1024
LEAN_LIMIT = 63 * 1024 * 1024 // 2
PAIR = 2 * GROUP
SHARES = (1, 5, 2)
ROW_TILE = 256


def load_table(tok_ref, raw, table, sems, rows):
    total, width = tok_ref.shape
    parts = total // rows
    copies = [
        pltpu.make_async_copy(tok_ref.at[pl.ds(p * rows, rows)], raw.at[pl.ds(p * rows, rows)], sems.at[p])
        for p in range(parts)
    ]
    for copy in copies:
        copy.start()
    for p in range(parts):
        copies[p].wait()

        def convert(g, carry):
            base = pl.multiple_of(p * rows + g * GROUP, GROUP)
            for k in range(width // LANES):
                x = raw[pl.ds(base, GROUP), k * LANES:(k + 1) * LANES].astype(jnp.float32)
                table[pl.ds(base * SUB + k, GROUP, stride=SUB), :] = x
            return carry

        lax.fori_loop(0, rows // GROUP, convert, 0, unroll=2)


def table_kernel(tok_ref, table, raw, sems):
    load_table(tok_ref, raw, table, sems, tok_ref.shape[0] // sems.shape[0])


def pick_rows(start, ask_refs, table, out_refs, stage, out_buf, out_sems):
    peers = len(ask_refs)
    block, width = out_refs[0].shape
    cap = ask_refs[0].shape[0] - LANES
    total = table.shape[0] // SUB - 1
    mask = 2 * total - 1

    def flush(j):
        return pltpu.make_async_copy(out_buf.at[j % 2], out_refs[j], out_sems.at[j % 2])

    for j, ask_ref in enumerate(ask_refs):
        if j >= 2:
            flush(j - 2).wait()
        live = jnp.clip(ask_ref[cap] - start, 0, block)

        def group(g, carry, j=j, ask_ref=ask_ref):
            base = pl.multiple_of(g * PAIR, PAIR)
            first = start + base
            slot = pl.multiple_of((g % 2) * PAIR * SUB, PAIR * SUB)
            for i in range(PAIR):
                row = ask_ref[first + i]
                if i % GROUP == 0:
                    row = row & mask
                stage[pl.ds(slot + i * SUB, SUB), :] = table[pl.ds(pl.multiple_of(row * SUB, SUB), SUB), :]
            for h in range(PAIR // GROUP):
                for k in range(width // LANES):
                    y = stage[pl.ds(slot + h * GROUP * SUB + k, GROUP, stride=SUB), :]
                    out_buf[j % 2, pl.ds(base + h * GROUP, GROUP), k * LANES:(k + 1) * LANES] = y.astype(jnp.bfloat16)
            return carry

        lax.fori_loop(0, pl.cdiv(live, PAIR), group, 0)
        flush(j).start()
    for j in range(peers - 2, peers):
        flush(j).wait()


def first_gather_kernel(start, peers, *refs):
    pick_rows(start, refs[:peers], refs[peers], refs[peers + 1:2 * peers + 1], *refs[2 * peers + 1:])


def gather_kernel(start, peers, *refs):
    tok_ref = refs[peers]
    raw, table, stage, out_buf, sems, out_sems = refs[2 * peers + 1:]
    load_table(tok_ref, raw, table, sems, tok_ref.shape[0] // sems.shape[0])
    pick_rows(start, refs[:peers], table, refs[peers + 1:2 * peers + 1], stage, out_buf, out_sems)


def ffn_kernel(bound_ref, gate_ref, win_ref, wout_ref, *refs):
    experts, width, inner = win_ref.shape
    peers = bound_ref.shape[0]
    x_refs, out_refs = refs[:peers], refs[peers:2 * peers]
    xs, outs, w1, w2, hidden, sems, x_sems, out_sems = refs[2 * peers:]
    tile = hidden.shape[0]
    cut = 512

    def fetch(e, slot):
        return (pltpu.make_async_copy(win_ref.at[e], w1.at[slot], sems.at[0, slot]),
                pltpu.make_async_copy(wout_ref.at[e], w2.at[slot], sems.at[1, slot]))

    def bring(s):
        return pltpu.make_async_copy(x_refs[s], xs.at[s], x_sems.at[s])

    def flush(s):
        return pltpu.make_async_copy(outs.at[s], out_refs[s], out_sems.at[s])

    bring(0).start()
    for copy in fetch(0, 0):
        copy.start()
    for s in range(1, peers):
        bring(s).start()

    def per_expert(e, carry):
        slot = e % 2
        for copy in fetch(e, slot):
            copy.wait()

        @pl.when(e + 1 < experts)
        def _():
            for copy in fetch(e + 1, 1 - slot):
                copy.start()

        def per_peer(s, carry2):
            @pl.when(e == 0)
            def _():
                pltpu.make_async_copy(x_refs[0], xs.at[s], x_sems.at[s]).wait()

            lo = bound_ref[s, e]
            hi = bound_ref[s, e + 1]
            first = lo // tile
            last = jnp.where(hi > lo, pl.cdiv(hi, tile), first)

            def per_tile(t, carry3):
                base = pl.multiple_of(t * tile, tile)
                x = xs[s, pl.ds(base, tile), :]
                for f in range(inner // cut):
                    pre = jnp.dot(x, w1[slot, :, f * cut:(f + 1) * cut], preferred_element_type=jnp.float32)
                    hidden[:, f * cut:(f + 1) * cut] = jax.nn.gelu(pre, approximate=True).astype(jnp.bfloat16)
                o = jnp.dot(hidden[...], w2[slot], preferred_element_type=jnp.float32)
                p = (gate_ref[s, pl.ds(base, tile), :] * o).astype(jnp.bfloat16).astype(jnp.float32)
                pos = base + lax.broadcasted_iota(jnp.int32, (tile, 1), 0)
                mine = (pos >= lo) & (pos < hi)
                old = outs[s, pl.ds(base, tile), :].astype(jnp.float32)
                outs[s, pl.ds(base, tile), :] = jnp.where(mine, p, old).astype(jnp.bfloat16)
                return carry3

            lax.fori_loop(first, last, per_tile, 0)
            for j in range(peers):
                @pl.when((e == experts - 1) & (s == j))
                def _():
                    flush(j).start()

            return carry2

        return lax.fori_loop(0, peers, per_peer, carry)

    lax.fori_loop(0, experts, per_expert, 0)
    for s in range(peers):
        flush(s).wait()


def add_rows(start, ask_refs, back_refs, table, stage, rows_buf, row_sems):
    peers = len(back_refs)
    block, width = back_refs[0].shape
    cap = ask_refs[0].shape[0] - LANES
    mask = 2 * (table.shape[0] // SUB - 1) - 1

    slots = rows_buf.shape[0]

    def fetch(j):
        return pltpu.make_async_copy(back_refs[j], rows_buf.at[j % slots, pl.ds(0, block)], row_sems.at[j % slots])

    def prime():
        for j in range(slots):
            fetch(j).start()

    def per_peer(j):
        ask_ref = ask_refs[j]
        slot = j % slots
        fetch(j).wait()
        live = jnp.clip(ask_ref[cap] - start, 0, block)

        def group(g, carry2):
            base = pl.multiple_of(g * PAIR, PAIR)
            for h in range(PAIR // GROUP):
                for k in range(width // LANES):
                    y = rows_buf[slot, pl.ds(base + h * GROUP, GROUP), k * LANES:(k + 1) * LANES]
                    stage[pl.ds(h * GROUP * SUB + k, GROUP, stride=SUB), :] = y.astype(jnp.float32)
            first = start + base
            asks = [ask_ref[first + i] for i in range(PAIR)]
            mixed = asks[0] > mask
            for h in range(1, PAIR // GROUP):
                mixed = jnp.logical_or(mixed, asks[h * GROUP] > mask)
            spots = [pl.ds(pl.multiple_of(((a & mask) if i % GROUP == 0 else a) * SUB, SUB), SUB)
                     for i, a in enumerate(asks)]

            @pl.when(jnp.logical_not(mixed))
            def _():
                for h in range(PAIR // GROUP):
                    ids = range(h * GROUP, (h + 1) * GROUP)
                    sums = [table[spots[i], :] + stage[i * SUB:(i + 1) * SUB, :] for i in ids]
                    for i, v in zip(ids, sums):
                        table[spots[i], :] = v

            @pl.when(mixed)
            def _():
                for i in range(PAIR):
                    table[spots[i], :] = table[spots[i], :] + stage[i * SUB:(i + 1) * SUB, :]

            return carry2

        lax.fori_loop(0, pl.cdiv(live, PAIR), group, 0)
        if j + slots < peers:
            fetch(j + slots).start()

    def run():
        for j in range(peers):
            per_peer(j)

    return prime, run


def first_combine_kernel(chunks, peers, *refs):
    ask_refs, tok_ref = refs[:peers], refs[peers]
    total, _ = tok_ref.shape
    count = peers * len(chunks)
    back_refs = refs[peers + 1:peers + 1 + count]
    table, raw, stage, rows_buf, sems, row_sems = refs[peers + 1 + count:]
    runs = [add_rows(start, ask_refs, back_refs[n * peers:(n + 1) * peers], table, stage, rows_buf, row_sems)
            for n, (start, _) in enumerate(chunks)]
    runs[0][0]()
    load_table(tok_ref, raw, table, sems, total // sems.shape[0])
    for n, (prime, run) in enumerate(runs):
        if n > 0:
            prime()
        run()


def last_combine_kernel(start, peers, *refs):
    ask_refs, table, back_refs = refs[:peers], refs[peers], refs[peers + 1:2 * peers + 1]
    out_ref, stage, rows_buf, out_buf, row_sems, out_sems = refs[2 * peers + 1:]
    total, width = out_ref.shape
    prime, run = add_rows(start, ask_refs, back_refs, table, stage, rows_buf, row_sems)
    prime()
    run()
    step = out_buf.shape[1]

    def flush(p, slot):
        return pltpu.make_async_copy(out_buf.at[slot], out_ref.at[pl.ds(p * step, step)], out_sems.at[slot])

    def write(p, carry):
        slot = p % 2

        @pl.when(p >= 2)
        def _():
            flush(p - 2, slot).wait()

        def convert(g, carry2):
            base = pl.multiple_of(g * GROUP, GROUP)
            for k in range(width // LANES):
                y = table[pl.ds((p * step + base) * SUB + k, GROUP, stride=SUB), :]
                out_buf[slot, pl.ds(base, GROUP), k * LANES:(k + 1) * LANES] = y.astype(jnp.bfloat16)
            return carry2

        lax.fori_loop(0, step // GROUP, convert, 0, unroll=4)
        flush(p, slot).start()
        return carry

    n_steps = total // step
    lax.fori_loop(0, n_steps, write, 0)
    for p in range(max(0, n_steps - 2), n_steps):
        flush(p, p % 2).wait()


def solution(mesh):
    peers = mesh.shape["ep"]
    chips = peers // 2
    row_spec = P(("dp", "ep"), None)
    expert_spec = P("ep", None, None)
    smem = pl.BlockSpec(memory_space=pltpu.SMEM)
    hbm = pl.BlockSpec(memory_space=pl.ANY)
    vmem = pl.BlockSpec(memory_space=pltpu.VMEM)
    params = pltpu.CompilerParams(vmem_limit_bytes=VMEM_LIMIT)
    lean = pltpu.CompilerParams(vmem_limit_bytes=LEAN_LIMIT)

    def local_layer(tok, sel, gate, win, wout):
        rows, width = tok.shape
        experts, slots = sel.shape
        inner = win.shape[2]
        total = experts * slots
        cap = 2 * total // peers
        parts = 8
        chunks = []
        for share in SHARES:
            chunks.append((sum(n for _, n in chunks), share * cap // 8))

        hops = [(0, 0), (1, 0), (1, 1), (chips - 1, 0), (chips - 1, 1), (0, 1)]
        hops += [(n, f) for n in range(2, chips - 1) for f in range(2)]
        me = lax.axis_index("ep")
        device = sel // rows
        code = (me // 2 + chips - device // 2) % chips * 2 + (me + device) % 2
        owner = sum(jnp.where(code == 2 * n + f, j, 0) for j, (n, f) in enumerate(hops))

        lane_e = lax.broadcasted_iota(jnp.int32, (experts, slots), 0)
        key = ((owner * (experts + 1) + lane_e) * rows + sel % rows).reshape(total)
        peer_ids = jnp.arange(peers, dtype=jnp.int32)
        counts = jnp.sum((owner.reshape(1, total) == peer_ids[:, None]).astype(jnp.int32), axis=1)
        fill_end = jnp.cumsum(cap - counts)
        fill_id = jnp.arange(peers * cap - total, dtype=jnp.int32)
        fill_owner = jnp.sum((fill_id[None, :] >= fill_end[:, None]).astype(jnp.int32), axis=0)
        fill_key = (fill_owner * (experts + 1) + experts) * rows + fill_id % rows
        keys, gates = lax.sort(
            (jnp.concatenate([key, fill_key]), jnp.concatenate([gate.reshape(total), jnp.zeros(fill_id.shape, jnp.float32)])),
            num_keys=1, is_stable=False)
        keys = keys.reshape(peers, cap)
        local = keys - peer_ids[:, None] * ((experts + 1) * rows)
        edges = jnp.arange(experts + 1, dtype=jnp.int32) * rows
        bounds = jnp.sum((local[:, None, :] < edges[None, :, None]).astype(jnp.int32), axis=2)
        which = local // rows
        lane = lax.broadcasted_iota(jnp.int32, (peers, cap), 1)
        mixed = (lane % GROUP == 0) & (which != jnp.roll(which, 1 - GROUP, axis=1))
        want = jnp.where(which < experts, local % rows, rows) + jnp.where(mixed, 2 * rows, 0)

        want = jnp.concatenate([want, jnp.broadcast_to(bounds[:, experts:], (peers, LANES))], axis=1)

        def exchange(xs, forward, pin=True):
            ys = list(xs)
            for j, (n, f) in enumerate(hops):
                there = [(i // 2 + n) % chips * 2 + (i % 2 + f) % 2 for i in range(peers)]
                pairs = [(i, k) if forward else (k, i) for i, k in enumerate(there)]
                if (n, f) != (0, 0):
                    y = lax.ppermute(xs[j], "ep", pairs)
                    ys[j] = pltpu.with_memory_space_constraint(y, pltpu.HBM) if pin else y
            return ys

        asked = exchange([want[j] for j in range(peers)], False, pin=False)

        def blocks(c):
            return [pltpu.HBM((chunks[c][1], width), jnp.bfloat16)] * peers

        table_type = pltpu.VMEM(((rows + 1) * SUB, LANES), jnp.float32)
        raw_type = pltpu.VMEM((rows, width), jnp.bfloat16)
        stage_type = pltpu.VMEM((2 * PAIR * SUB, LANES), jnp.float32)
        two = pltpu.SemaphoreType.DMA((2,))

        table = pl.pallas_call(
            table_kernel,
            out_shape=table_type,
            in_specs=[hbm],
            out_specs=vmem,
            scratch_shapes=[raw_type, pltpu.SemaphoreType.DMA((parts,))],
            compiler_params=lean,
            cost_estimate=pl.CostEstimate(flops=10_000_000_000, bytes_accessed=2 * rows * width, transcendentals=0),
            name="row_table",
        )(tok)

        def gather(c, after):
            start, block = chunks[c]
            first = after is None
            turn = asked if first else lax.optimization_barrier((*asked, after))[:peers]
            buffers = [stage_type, pltpu.VMEM((2, block, width), jnp.bfloat16)]
            if not first:
                buffers = [raw_type, table_type] + buffers + [pltpu.SemaphoreType.DMA((parts,))]
            return pl.pallas_call(
                functools.partial(first_gather_kernel if first else gather_kernel, start, peers),
                out_shape=blocks(c),
                in_specs=[smem] * peers + [vmem if first else hbm],
                out_specs=[hbm] * peers,
                scratch_shapes=buffers + [two],
                compiler_params=lean if first else params,
                cost_estimate=pl.CostEstimate(flops=15_000_000_000, bytes_accessed=3 * rows * width, transcendentals=0),
                name="gather_rows",
            )(*turn, pltpu.with_memory_space_constraint(table, pltpu.VMEM) if first else tok)

        def ffn(c, x):
            start, block = chunks[c]
            cb = jnp.clip(bounds - start, 0, block)
            g = gates[:, start:start + block].reshape(peers, block, 1)
            return pl.pallas_call(
                ffn_kernel,
                out_shape=blocks(c),
                in_specs=[smem, vmem, hbm, hbm] + [hbm] * peers,
                out_specs=[hbm] * peers,
                scratch_shapes=[
                    pltpu.VMEM((peers, block, width), jnp.bfloat16),
                    pltpu.VMEM((peers, block, width), jnp.bfloat16),
                    pltpu.VMEM((2, width, inner), jnp.bfloat16),
                    pltpu.VMEM((2, inner, width), jnp.bfloat16),
                    pltpu.VMEM((min(ROW_TILE, block), inner), jnp.bfloat16),
                    pltpu.SemaphoreType.DMA((2, 2)),
                    pltpu.SemaphoreType.DMA((peers,)),
                    pltpu.SemaphoreType.DMA((peers,)),
                ],
                compiler_params=params,
                cost_estimate=pl.CostEstimate(
                    flops=4 * total * width * inner // len(chunks), bytes_accessed=4 * experts * width * inner,
                    transcendentals=total * inner // len(chunks)),
                name="expert_ffn",
            )(cb, g, win, wout, *x)

        sent = []
        for c in range(len(chunks)):
            sent.append(gather(c, sent[-1][0] if sent else None))
        inputs = [exchange(x, True) for x in sent]
        bounds, gates = lax.optimization_barrier((bounds, gates, inputs[0][1]))[:2]
        gates = gates.reshape(peers, cap)
        done = [ffn(c, x) for c, x in enumerate(inputs)]
        back = [exchange(x, False) for x in done]

        early, last = chunks[:-1], chunks[-1]
        step = rows // parts
        sums = pl.pallas_call(
            functools.partial(first_combine_kernel, early, peers),
            out_shape=table_type,
            in_specs=[smem] * peers + [hbm] + [hbm] * (peers * len(early)),
            out_specs=vmem,
            scratch_shapes=[
                raw_type, stage_type, pltpu.VMEM((2, max(n for _, n in early), width), jnp.bfloat16),
                pltpu.SemaphoreType.DMA((parts,)), two,
            ],
            compiler_params=lean,
            cost_estimate=pl.CostEstimate(flops=40_000_000_000, bytes_accessed=6 * rows * width, transcendentals=0),
            name="combine_first",
        )(*asked, tok, *[x for xs in back[:-1] for x in xs])
        return pl.pallas_call(
            functools.partial(last_combine_kernel, last[0], peers),
            out_shape=jax.ShapeDtypeStruct((rows, width), jnp.bfloat16),
            in_specs=[smem] * peers + [vmem] + [hbm] * peers,
            out_specs=hbm,
            scratch_shapes=[
                stage_type, pltpu.VMEM((peers, last[1], width), jnp.bfloat16),
                pltpu.VMEM((2, step, width), jnp.bfloat16), pltpu.SemaphoreType.DMA((peers,)), two,
            ],
            compiler_params=lean,
            cost_estimate=pl.CostEstimate(flops=20_000_000_000, bytes_accessed=6 * rows * width, transcendentals=0),
            name="combine_last",
        )(*asked, pltpu.with_memory_space_constraint(sums, pltpu.VMEM), *back[-1])

    return jax.shard_map(
        local_layer, mesh=mesh, in_specs=(row_spec, row_spec, row_spec, expert_spec, expert_spec),
        out_specs=row_spec, check_vma=False)
```
